32 devices in a mesh: gx: 4 (over z), gy: 2 (over x), gz: 4 (over y, core).
Axes of the slice: x: 2, y: 2, z: 4, core: 2. Of those that a mesh axis runs over, the one named last changes fastest.
Arguments:
- block_x: float32 [16, 24, 12, 512], P(None, 'gz', 'gy', 'gx')
- block_hx: float32 [16, 24, 12, 512], P(None, 'gz', 'gy', 'gx')
- block_p: float32 [16, 24, 12, 512], P(None, 'gz', 'gy', 'gx')
- block_hp: float32 [16, 24, 12, 512], P(None, 'gz', 'gy', 'gx')
- potential: float32 [24, 12, 512], P('gz', 'gy', 'gx'), may hold values from -2 to 2
- projectors: float32 [4, 2, 4, 8, 4, 256], P('gz', 'gy', 'gx'), may hold values from -0.75 to 0.75
- coupling: float32 [4, 2, 4, 8, 4, 4], P('gz', 'gy', 'gx'), may hold values from 0.25 to 1.25
- atom_count: int32 [4, 2, 4], P('gz', 'gy', 'gx'), may hold values from 0 to 8, as said below
- proj_count: int32 [4, 2, 4, 8], P('gz', 'gy', 'gx'), may hold values from 1 to 4
- offsets: int32 [3, 4, 2, 4, 8], P(None, 'gz', 'gy', 'gx'), may hold values from 0 to 127, as said below
- extents: int32 [3, 4, 2, 4, 8], P(None, 'gz', 'gy', 'gx'), may hold values from 2 to 16, as said below
Outputs:
- w_block: float32 [16, 24, 12, 512], P(None, 'gz', 'gy', 'gx')
- hw_block: float32 [16, 24, 12, 512], P(None, 'gz', 'gy', 'gx')
- gram: float32 [48, 48], replicated
- rayleigh: float32 [48, 48], replicated
The draws below stay inside these ranges and needn't reach their ends.
Inputs may be any that keep to these rules, and one draw needn't show every extreme that they name: `atom_count`: slots at and above a domain's count are empty; some domain is full in every draw. The first proj_count projectors of a slot are used. `offsets`: components z, y, x are below 6, 6, 128. `extents`: components z, y, x are at most 4, 4, 16; some slot has the full box in every draw.
All inputs are finite; a program needn't handle non-finite values.
Results may differ from the reference program's by a relative error of at most 0.0003.
Values sent between devices are 32-bit elements; how exact they have to be, the bound alone decides.
A program may use at most 64 MiB of HBM per device.

```python
import math
import jax
import jax.numpy as jnp
from jax import lax

NCOL = 16
NPROJ = 4
CZ = 6
CY = 6
CX = 128
SLOTS = 8
BZ = 4
BY = 4
BX = 16
BOXC = 256
DOMAINS_Z = 4
DOMAINS_Y = 2
DOMAINS_X = 4
NZ = 24
NY = 12
NX = 512


def paired_fields(key, salt):
    base_key = jax.random.fold_in(key, salt)
    keys = jax.random.split(base_key, 6)
    shape = (NCOL, NZ, NY, NX)
    rough = jax.random.normal(keys[1], shape, jnp.float32)
    domain_scale = jnp.exp(jax.random.uniform(keys[2], (NZ // CZ, NY // CY, 1), jnp.float32, -1.2, 1.2))
    scale_field = jnp.repeat(jnp.repeat(domain_scale, CZ, axis=0), CY, axis=1)
    first_field = rough * scale_field[None]
    mixing = jnp.diag(jax.random.uniform(keys[3], (NCOL,), jnp.float32, 1.0, 4.0)) + 0.3 * jax.random.normal(keys[4], (NCOL, NCOL), jnp.float32) / math.sqrt(NCOL)
    second_field = jnp.einsum('kzyx,kj->jzyx', first_field, mixing) + 0.5 * jax.random.normal(keys[5], shape, jnp.float32) * scale_field[None]
    return (first_field, second_field)


def draw_block_x(key, part):
    return paired_fields(key, 11)[0]


def draw_block_hx(key, part):
    return paired_fields(key, 11)[1]


def draw_block_p(key, part):
    return paired_fields(key, 23)[0]


def draw_block_hp(key, part):
    return paired_fields(key, 23)[1]


def corner_slot():
    shape = (DOMAINS_Z, DOMAINS_Y, DOMAINS_X, SLOTS)
    total_slots = DOMAINS_Z * DOMAINS_Y * DOMAINS_X * SLOTS
    flat_index = jnp.arange(total_slots, dtype=jnp.int32).reshape(shape)
    return flat_index == total_slots - SLOTS


def draw_atom_count(key, part):
    keys = jax.random.split(jax.random.fold_in(key, 5), 4)
    shape = (DOMAINS_Z, DOMAINS_Y, DOMAINS_X)
    heavy_domain = jax.random.randint(keys[0], shape, 0, 4) == 0
    large_count = jax.random.randint(keys[1], shape, SLOTS // 2, SLOTS + 1)
    small_count = jax.random.randint(keys[2], shape, 0, SLOTS // 4 + 1)
    counts = jnp.where(heavy_domain, large_count, small_count)
    domain_total = DOMAINS_Z * DOMAINS_Y * DOMAINS_X
    chosen = jax.random.randint(keys[3], (), 0, domain_total)
    flat_index = jnp.arange(domain_total, dtype=jnp.int32).reshape(shape)
    full_domain = (flat_index == chosen) | (flat_index == domain_total - 1)
    return jnp.where(full_domain, SLOTS, counts).astype(jnp.int32)


def draw_offsets(key, part):
    keys = jax.random.split(jax.random.fold_in(key, 31), 3)
    shape = (DOMAINS_Z, DOMAINS_Y, DOMAINS_X, SLOTS)
    edge_slot = corner_slot()
    along_z = jnp.where(edge_slot, CZ - 1, jax.random.randint(keys[0], shape, 0, CZ))
    along_y = jnp.where(edge_slot, CY - 1, jax.random.randint(keys[1], shape, 0, CY))
    along_x = jnp.where(edge_slot, CX - 1, jax.random.randint(keys[2], shape, 0, CX))
    return jnp.stack([along_z, along_y, along_x]).astype(jnp.int32)


def draw_extents(key, part):
    keys = jax.random.split(jax.random.fold_in(key, 47), 4)
    shape = (DOMAINS_Z, DOMAINS_Y, DOMAINS_X, SLOTS)
    total_slots = DOMAINS_Z * DOMAINS_Y * DOMAINS_X * SLOTS
    chosen = jax.random.randint(keys[3], (), 0, total_slots)
    flat_index = jnp.arange(total_slots, dtype=jnp.int32).reshape(shape)
    full_box = (flat_index == chosen) | corner_slot()
    along_z = jnp.where(full_box, BZ, jax.random.randint(keys[0], shape, 2, BZ + 1))
    along_y = jnp.where(full_box, BY, jax.random.randint(keys[1], shape, 2, BY + 1))
    along_x = jnp.where(full_box, BX, jax.random.randint(keys[2], shape, 2, BX + 1))
    return jnp.stack([along_z, along_y, along_x]).astype(jnp.int32)


def place_ends(array, rng, low, top_value):
    dims = array.shape
    index_at = [jax.random.randint(jax.random.fold_in(rng, axis), (), 0, dims[axis]) for axis in range(len(dims))]
    array = array.at[tuple(index_at)].set(low)
    longest = dims.index(max(dims))
    index_at[longest] = (index_at[longest] + 1) % dims[longest]
    return array.at[tuple(index_at)].set(top_value)


def block_levels(own_key, extent, cuts, low, largest):
    gain, own = 1.0, jax.random.fold_in(own_key, 6)
    for axis_at, blocks in cuts:
        heights = jnp.exp(jax.random.uniform(jax.random.fold_in(own, axis_at), (blocks,), jnp.float32, low / len(cuts), largest / len(cuts)))
        gain = gain * jnp.repeat(heights, extent[axis_at] // blocks).reshape([-1 if axis == axis_at else 1 for axis in range(len(extent))])
    return gain


def gaussian(stream_key, dims, scale, bound, pieces=(), kind=jnp.bfloat16):
    values = scale * jax.random.normal(stream_key, dims, jnp.float32)
    if pieces:
        values = values * block_levels(stream_key, dims, pieces, -0.22, 0.18)
    return jnp.clip(values, -bound, bound).astype(kind)


def setup_inputs(seed: int = 0) -> dict:
    splits = jax.random.split(jax.random.key(seed), 12)
    block_x = draw_block_x(jax.random.fold_in(splits[11], 71), 0)
    block_hx = draw_block_hx(jax.random.fold_in(splits[11], 71), 0)
    block_p = draw_block_p(jax.random.fold_in(splits[11], 71), 0)
    block_hp = draw_block_hp(jax.random.fold_in(splits[11], 71), 0)
    potential = jnp.clip(jax.random.uniform(splits[4], (NZ, NY, NX), jnp.float32, -2.0, 2.0) * block_levels(splits[4], (NZ, NY, NX), ((0, 4), (1, 2), (2, 4)), -0.4, 0.0), -2.0, 2.0)
    projectors = gaussian(splits[5], (DOMAINS_Z, DOMAINS_Y, DOMAINS_X, SLOTS, NPROJ, BOXC), 0.125, 0.75, ((0, 4), (1, 2), (2, 4)), jnp.float32)
    coupling = jnp.clip(0.25 + 1.0 * jax.random.uniform(splits[6], (DOMAINS_Z, DOMAINS_Y, DOMAINS_X, SLOTS, NPROJ, NPROJ), jnp.float32) ** block_levels(splits[6], (DOMAINS_Z, DOMAINS_Y, DOMAINS_X, SLOTS, NPROJ, NPROJ), ((0, 4), (1, 2), (2, 4)), -0.2, 0.2), 0.25, 1.25)
    atom_count = draw_atom_count(jax.random.fold_in(splits[11], 71), 0)
    proj_count = place_ends(jax.random.randint(splits[8], (DOMAINS_Z, DOMAINS_Y, DOMAINS_X, SLOTS), 1, NPROJ + 1), jax.random.fold_in(splits[8], 1), 1, NPROJ).astype(jnp.int32)
    offsets = draw_offsets(jax.random.fold_in(splits[11], 71), 0)
    extents = draw_extents(jax.random.fold_in(splits[11], 71), 0)
    return {"block_x": block_x, "block_hx": block_hx, "block_p": block_p, "block_hp": block_hp, "potential": potential, "projectors": projectors, "coupling": coupling, "atom_count": atom_count, "proj_count": proj_count, "offsets": offsets, "extents": extents}


LAP_CENTER = -5369.0 / 1800.0
LAP_COEFFS = (12.0 / 7.0, -15.0 / 56.0, 10.0 / 189.0, -1.0 / 112.0, 2.0 / 1925.0, -1.0 / 16632.0)
HIGHEST = lax.Precision.HIGHEST

def masked_projectors(projectors, atom_count, proj_count, extents):
    slot_index = jnp.arange(projectors.shape[-3], dtype=jnp.int32)
    live_slot = slot_index < atom_count[..., None]
    proj_index = jnp.arange(projectors.shape[-2], dtype=jnp.int32)
    live_proj = proj_index < proj_count[..., None]
    cell_index = jnp.arange(projectors.shape[-1], dtype=jnp.int32)
    along_z = cell_index // (BY * BX)
    along_y = cell_index // BX % BY
    along_x = cell_index % BX
    inside = (along_z < extents[0][..., None]) & (along_y < extents[1][..., None]) & (along_x < extents[2][..., None])
    keeper = live_slot[..., None, None] & live_proj[..., None] & inside[..., None, :]
    return jnp.where(keeper, projectors, jnp.zeros_like(projectors))

def kinetic_term(column_block):
    summed = 3.0 * LAP_CENTER * column_block
    for distance, weight in enumerate(LAP_COEFFS, start=1):
        for axis_number in (1, 2, 3):
            summed = summed + weight * (jnp.roll(column_block, distance, axis_number) + jnp.roll(column_block, -distance, axis_number))
    return -0.5 * summed

def nonlocal_term(column_block, beta_masked, sym_coupling, offsets):
    columns = column_block.shape[0]
    start_z = jnp.arange(DOMAINS_Z, dtype=jnp.int32)[:, None, None, None] * CZ + offsets[0]
    start_y = jnp.arange(DOMAINS_Y, dtype=jnp.int32)[None, :, None, None] * CY + offsets[1]
    start_x = jnp.arange(DOMAINS_X, dtype=jnp.int32)[None, None, :, None] * CX + offsets[2]
    cell_index = jnp.arange(BZ * BY * BX, dtype=jnp.int32)
    grid_z = (start_z[..., None] + cell_index // (BY * BX)) % NZ
    grid_y = (start_y[..., None] + cell_index // BX % BY) % NY
    grid_x = (start_x[..., None] + cell_index % BX) % NX
    flat_index = ((grid_z * NY + grid_y) * NX + grid_x).astype(jnp.int32)
    flat_block = column_block.reshape(columns, NZ * NY * NX)
    gathered = flat_block[:, flat_index]
    correlations = jnp.einsum('abcspk,nabcsk->abcspn', beta_masked, gathered, precision=HIGHEST)
    weights_out = jnp.einsum('abcspq,abcsqn->abcspn', sym_coupling, correlations, precision=HIGHEST)
    spread = jnp.einsum('abcspk,abcspn->nabcsk', beta_masked, weights_out, precision=HIGHEST)
    result = jnp.zeros_like(flat_block).at[:, flat_index.reshape(-1)].add(spread.reshape(columns, -1))
    return result.reshape(column_block.shape)

def inner_product(left_block, right_block, cell_weight):
    left_flat = left_block.reshape(left_block.shape[0], -1)
    right_flat = right_block.reshape(right_block.shape[0], -1)
    return jnp.einsum('ic,jc->ij', left_flat, right_flat, precision=HIGHEST) * cell_weight

def reference(block_x, block_hx, block_p, block_hp, potential, projectors, coupling, atom_count, proj_count, offsets, extents):
    cell_weight = 1.0 / (NZ * NY * NX)
    beta_masked = masked_projectors(projectors, atom_count, proj_count, extents)
    sym_coupling = 0.5 * (coupling + jnp.swapaxes(coupling, -1, -2))
    correlation = inner_product(block_x, block_x, cell_weight)
    projected = inner_product(block_x, block_hx, cell_weight)
    factor = jnp.linalg.cholesky(correlation)
    ritz_theta = jax.scipy.linalg.cho_solve((factor, True), projected)
    residual = block_hx - jnp.einsum('kzyx,kj->jzyx', block_x, ritz_theta, precision=HIGHEST)
    w_block = residual / (1.0 + potential * potential)
    hw_block = kinetic_term(w_block) + potential * w_block + nonlocal_term(w_block, beta_masked, sym_coupling, offsets)
    search_space = (block_x, w_block, block_p)
    images = (block_hx, hw_block, block_hp)
    gram = jnp.concatenate([jnp.concatenate([inner_product(left_block, right_block, cell_weight) for right_block in search_space], axis=1) for left_block in search_space], axis=0)
    rayleigh = jnp.concatenate([jnp.concatenate([inner_product(left_block, right_block, cell_weight) for right_block in images], axis=1) for left_block in search_space], axis=0)
    return (w_block, hw_block, gram, rayleigh)
```

```python
import functools

import jax
import jax.numpy as jnp
from jax import lax
from jax.experimental import pallas as pl
from jax.experimental.pallas import tpu as pltpu
from jax.sharding import PartitionSpec as P

BZ, BY, BX = 4, 4, 16
LAP_CENTER = -5369.0 / 1800.0
LAP_COEFFS = (12.0 / 7.0, -15.0 / 56.0, 10.0 / 189.0, -1.0 / 112.0, 2.0 / 1925.0, -1.0 / 16632.0)
MESH = pl.DeviceIdType.MESH
AXES = ("gz", "gy", "gx")
F32 = jnp.float32
BF16 = jnp.bfloat16
HX, HP, XX, PP, WW, HW = range(6)


def masked_projectors(projectors, atom_count, proj_count, extents):
    slot_index = jnp.arange(projectors.shape[-3], dtype=jnp.int32)
    live_slot = slot_index < atom_count[..., None]
    proj_index = jnp.arange(projectors.shape[-2], dtype=jnp.int32)
    live_proj = proj_index < proj_count[..., None]
    cell_index = jnp.arange(projectors.shape[-1], dtype=jnp.int32)
    along_z = cell_index // (BY * BX)
    along_y = cell_index // BX % BY
    along_x = cell_index % BX
    inside = (
        (along_z < extents[0][..., None])
        & (along_y < extents[1][..., None])
        & (along_x < extents[2][..., None])
    )
    keeper = live_slot[..., None, None] & live_proj[..., None] & inside[..., None, :]
    return jnp.where(keeper, projectors, jnp.zeros_like(projectors))


def tiles_of(count):
    return -(-count // 8)


def kernel(
    sizes, groups, dims,
    off_ref, d_ref, x_ref, hx_ref, p_ref, hp_ref, v_ref, beta_ref,
    w_ref, hw_ref, red1_ref, red2_ref,
    stack, zext, ybuf, zybuf, plow, phigh, xr, xl, frame, frame_x, halo_x,
    blo, bhi, pieces, nf, nh, spack, rz, ry, rzy, rx, wout,
    *rest,
):
    cz, cy, cx, slots, nproj, cols = dims
    nz, ny, nx = sizes
    n_red = len(groups)
    bufs = (rest[:n_red], rest[n_red : 2 * n_red])
    rest = rest[2 * n_red :]
    red_send, red_recv, halo_send, halo_recv, spill_send, spill_recv = rest
    zi, yi, xi = (lax.axis_index(a) for a in AXES)
    size_of = dict(zip(AXES, sizes))
    here = dict(zip(AXES, (zi, yi, xi)))
    fz, fy = cz + BZ - 1, cy + BY - 1
    own = cz * cy
    lane = lax.broadcasted_iota(jnp.int32, (cols, 128), 1)

    def neighbour(dz, dy, dx):
        step = dict(zip(AXES, (dz, dy, dx)))
        return {a: lax.rem(here[a] + step[a] + size_of[a], size_of[a]) for a in AXES}

    def member(group, offset):
        total = 1
        index = 0
        for a in group:
            total *= size_of[a]
            index = index * size_of[a] + here[a]
        target = lax.rem(index + offset, total)
        device = {}
        for a in reversed(group):
            device[a] = lax.rem(target, size_of[a])
            target = target // size_of[a]
        return {a: device.get(a, here[a]) for a in AXES}, index, total

    octant = [(1, 0, 0), (0, 1, 0), (1, 1, 0), (0, 0, 1), (1, 0, 1), (0, 1, 1), (1, 1, 1)]
    barrier = pltpu.get_barrier_semaphore()
    greeted = 0
    for group in groups:
        total = member(group, 0)[2]
        for offset in range(1, total):
            pl.semaphore_signal(
                barrier, inc=1, device_id=member(group, offset)[0], device_id_type=MESH
            )
            greeted += 1
    for dz, dy, dx in octant:
        for sign in (1, -1):
            pl.semaphore_signal(
                barrier, inc=1, device_id=neighbour(sign * dz, sign * dy, sign * dx),
                device_id_type=MESH,
            )
            greeted += 1

    def split_store(kind, cell, value):
        high = value.astype(BF16)
        low = (value - high.astype(F32)).astype(BF16)
        start = cell * 128 if isinstance(cell, int) else pl.multiple_of(cell * 128, 128)
        stack[kind * 32 : kind * 32 + 32, pl.ds(start, 128)] = jnp.concatenate([high, low], 0)

    @pl.loop(0, own)
    def _(cell):
        split_store(HX, cell, hx_ref[cell])
        split_store(HP, cell, hp_ref[cell])
        split_store(XX, cell, x_ref[cell])
        split_store(PP, cell, p_ref[cell])

    def products(left, right_from, right_to):
        m = lax.dot_general(
            stack[left * 32 : left * 32 + 32, :],
            stack[right_from * 32 : right_to * 32, :],
            (((1,), (1,)), ((), ())),
            preferred_element_type=F32,
        )
        return m[:cols] + m[cols:]

    def reduced(which, payload):
        base = which * sum(member(g, 0)[2] for g in groups)
        for phase, group in enumerate(groups):
            buf = bufs[which][phase]
            _, index, total = member(group, 0)
            buf[index] = payload
            if phase == 0 and which == 0:
                pl.semaphore_wait(barrier, greeted)
            copies = []
            for offset in range(1, total):
                copies.append(
                    pltpu.make_async_remote_copy(
                        src_ref=buf.at[index],
                        dst_ref=buf.at[index],
                        send_sem=red_send.at[base + offset],
                        recv_sem=red_recv.at[base + offset],
                        device_id=member(group, offset)[0],
                        device_id_type=MESH,
                    )
                )
                copies[-1].start()
            base += total
            yield None
            for copy in copies:
                copy.wait()
            payload = buf[0]
            for slot in range(1, total):
                payload = payload + buf[slot]
        yield payload

    def finish(steps):
        out = None
        for out in steps:
            pass
        return out

    x_row = products(XX, HX, WW)
    hx_row = products(HX, HX, WW)
    p_row = products(PP, HX, WW)
    first = jnp.where(lane < 32, pltpu.roll(hx_row, 64, 1), x_row)
    reduction = reduced(0, jnp.concatenate([first, p_row], 0))
    next(reduction)

    lane64 = lax.broadcasted_iota(jnp.int32, (BZ * BY * nproj, 128), 1)
    per_slot = BZ * BY * nproj
    for s in range(slots):
        ox = off_ref[2 * slots + s]
        rolled = pltpu.roll(beta_ref[s * per_slot : (s + 1) * per_slot, :], ox, 1)
        blo[s * per_slot : (s + 1) * per_slot, :] = jnp.where(lane64 >= ox, rolled, 0.0)
        bhi[s * per_slot : (s + 1) * per_slot, :] = jnp.where(lane64 < ox, rolled, 0.0)
    rim_y = BY + 2
    rim = (BZ + 2) * rim_y

    @pl.loop(0, slots * rim)
    def _(i):
        pieces[i] = jnp.zeros(pieces.shape[1:], F32)

    sums1 = finish(reduction)
    red1_ref[...] = sums1
    folded = sums1[:cols] + pltpu.roll(sums1[:cols], 112, 1)
    matrix = jnp.concatenate([pltpu.roll(folded, 64, 1), folded], 0)
    lane2 = lax.broadcasted_iota(jnp.int32, (2 * cols, 128), 1)
    matrix = jnp.where(lane2 < cols, matrix, 0.0)
    for k in range(cols):
        row = matrix[k : k + 1, :]
        column = matrix[:, k : k + 1] / matrix[k : k + 1, k : k + 1]
        matrix = jnp.where(lane2 == k, column, matrix - column * row)
    theta_t = matrix[cols:, :]
    theta_cols = [jnp.broadcast_to(theta_t[:, k : k + 1], (cols, 128)) for k in range(cols)]

    @pl.loop(0, own)
    def _(cell):
        xs = x_ref[cell]
        value = hx_ref[cell]
        for k in range(cols):
            value = value - theta_cols[k] * xs[k : k + 1, :]
        vv = v_ref[cell]
        value = value / (1.0 + vv * vv)
        zext[own + cell] = value
        w_ref[cell] = value
        split_store(WW, cell, value)

    for q in range(tiles_of(own)):
        low = jnp.zeros((cols, 128), F32)
        high = low
        for j in range(min(8, own - 8 * q)):
            tile = zext[own + 8 * q + j]
            keep = (lane >= 16 * j) & (lane < 16 * j + 16)
            low = jnp.where(keep, pltpu.roll(tile, 16 * j, 1) if j else tile, low)
            high = jnp.where(keep, pltpu.roll(tile, (16 * j + 16) % 128, 1) if j < 7 else tile, high)
        plow[q] = low
        phigh[q] = high

    two_y = ny == 2
    mine = zext.at[pl.ds(own, own)]
    sends = [
        (mine, ybuf.at[1], (0, -1, 0)),
        (mine, zext.at[pl.ds(2 * own, own)], (-1, 0, 0)),
        (mine, zext.at[pl.ds(0, own)], (1, 0, 0)),
    ]
    if not two_y:
        sends.append((mine, ybuf.at[0], (0, 1, 0)))
    sends += [
        (plow, xr.at[0], (0, 0, -1)),
        (phigh, xl, (0, 0, 1)),
        (plow, xr.at[1], (-1, 0, -1)),
        (plow, xr.at[2], (0, -1, -1)),
        (plow, xr.at[3], (-1, -1, -1)),
        (zext.at[pl.ds(own, (BZ - 1) * cy)], zybuf, (-1, -1, 0)),
    ]

    def launch(sends, send_sem, recv_sem):
        copies = []
        for i, (source, target, where) in enumerate(sends):
            copies.append(
                pltpu.make_async_remote_copy(
                    src_ref=source,
                    dst_ref=target,
                    send_sem=send_sem.at[i],
                    recv_sem=recv_sem.at[i],
                    device_id=neighbour(*where),
                    device_id_type=MESH,
                )
            )
            copies[-1].start()
        return copies

    copies = launch(sends, halo_send, halo_recv)
    w_row = products(WW, HX, WW)
    w_row2 = products(WW, XX, HW)
    for copy in copies:
        copy.wait()

    below_y = 1 if two_y else 0
    for z in range(fz):
        for y in range(fy):
            up_z, up_y = z >= cz, y >= cy
            local = (z - cz * up_z) * cy + (y - cy * up_y)
            if up_z and up_y:
                tile = zybuf[local]
            elif up_z:
                tile = zext[2 * own + local]
            elif up_y:
                tile = ybuf[1, local]
            else:
                tile = zext[own + local]
            frame[z * fy + y] = tile
            shift = (128 - 16 * (local % 8)) % 128
            tile = xr[up_z + 2 * up_y, local // 8]
            tile = pltpu.roll(tile, shift, 1) if shift else tile
            frame_x[z * fy + y] = tile
            if not up_z and not up_y:
                left = xl[local // 8]
                turn = (112 - 16 * (local % 8)) % 128
                left = pltpu.roll(left, turn, 1) if turn else left
                halo_x[local] = jnp.where(lane < 64, tile, left)

    @pl.loop(0, slots)
    def _(s):
        oz, oy = off_ref[s], off_ref[slots + s]
        sums = [jnp.zeros((cols, 128), F32) for _ in range(nproj)]
        for a in range(BZ):
            for b in range(BY):
                at = (oz + a) * fy + oy + b
                tile, tile_x = frame[at], frame_x[at]
                base = s * per_slot + (a * BY + b) * nproj
                for q in range(nproj):
                    sums[q] = sums[q] + tile * blo[pl.ds(base + q, 1), :]
                    sums[q] = sums[q] + jnp.where(
                        lane < 16, tile_x * bhi[pl.ds(base + q, 1), :], 0.0
                    )
        overlaps = [jnp.broadcast_to(jnp.sum(v, axis=1, keepdims=True), (cols, 128)) for v in sums]
        outs = []
        for p in range(nproj):
            value = overlaps[0] * d_ref[(s * nproj + p) * nproj]
            for q in range(1, nproj):
                value = value + overlaps[q] * d_ref[(s * nproj + p) * nproj + q]
            outs.append(value)
        for a in range(BZ):
            for b in range(BY):
                base = s * per_slot + (a * BY + b) * nproj
                low = outs[0] * blo[pl.ds(base, 1), :]
                high = outs[0] * bhi[pl.ds(base, 1), :]
                for p in range(1, nproj):
                    low = low + outs[p] * blo[pl.ds(base + p, 1), :]
                    high = high + outs[p] * bhi[pl.ds(base + p, 1), :]
                place = s * rim + (a + 1) * rim_y + b + 1
                pieces[place, 0] = low
                pieces[place, 1] = high

    @pl.loop(0, fz)
    def _(z):
        starts = []
        for s in range(slots):
            a = jnp.minimum(jnp.maximum(z - off_ref[s], -1), BZ) + 1
            starts.append(s * rim + a * rim_y)
        for y in range(fy):
            low = jnp.zeros((cols, 128), F32)
            high = low
            for s in range(slots):
                b = jnp.minimum(jnp.maximum(y - off_ref[slots + s], -1), BY) + 1
                low = low + pieces[starts[s] + b, 0]
                high = high + pieces[starts[s] + b, 1]
            nf[z, y] = low
            nh[z, y] = high

    spans = []
    filled = 0
    for up_z in (0, 1):
        for up_y in (0, 1):
            cells = [
                (z, y)
                for z in (range(cz, fz) if up_z else range(cz))
                for y in (range(cy, fy) if up_y else range(cy))
            ]
            spans.append((filled, up_z, up_y, cells))
            for q in range(tiles_of(len(cells))):
                tile = jnp.zeros((cols, 128), F32)
                for j, (z, y) in enumerate(cells[8 * q : 8 * q + 8]):
                    keep = (lane >= 16 * j) & (lane < 16 * j + 16)
                    value = nh[z, y]
                    tile = jnp.where(keep, pltpu.roll(value, 16 * j, 1) if j else value, tile)
                spack[filled + q] = tile
            filled += tiles_of(len(cells))
    more_z, more_y = fz - cz, fy - cy
    sends = [
        (nf.at[pl.ds(cz, more_z), pl.ds(0, cy)], rz, (1, 0, 0)),
        (nf.at[pl.ds(0, cz), pl.ds(cy, more_y)], ry, (0, 1, 0)),
        (nf.at[pl.ds(cz, more_z), pl.ds(cy, more_y)], rzy, (1, 1, 0)),
    ]
    for begin, up_z, up_y, cells in spans:
        part = pl.ds(begin, tiles_of(len(cells)))
        sends.append((spack.at[part], rx.at[part], (up_z, up_y, 1)))
    copies = launch(sends, spill_send, spill_recv)

    @pl.loop(0, cz)
    def _(z):
        for y in range(cy):
            cell = z * cy + y
            centre = zext[own + cell]
            edge = halo_x[cell]
            vv = v_ref[cell]
            total = centre * (vv - 1.5 * LAP_CENTER)
            for k, weight in enumerate(LAP_COEFFS, start=1):
                beside = zext[own + cell + k * cy] + zext[own + cell - k * cy]
                for target in (y + k, y - k):
                    if target >= cy:
                        beside = beside + ybuf[1, z * cy + target - cy]
                    elif target < 0:
                        beside = beside + ybuf[below_y, z * cy + target + cy]
                    else:
                        beside = beside + zext[own + z * cy + target]
                beside = beside + pltpu.roll(jnp.where(lane < k, edge, centre), 128 - k, 1)
                beside = beside + pltpu.roll(jnp.where(lane >= 128 - k, edge, centre), k, 1)
                total = total - 0.5 * weight * beside
            hw_ref[cell] = total + nf[z, y]

    for copy in copies:
        copy.wait()
    for z in range(cz):
        for y in range(cy):
            cell = z * cy + y
            value = hw_ref[cell]
            if z < more_z:
                value = value + rz[z, y]
            if y < more_y:
                value = value + ry[z, y]
            if z < more_z and y < more_y:
                value = value + rzy[z, y]
            extra = None
            for begin, up_z, up_y, cells in spans:
                where = (z + cz * up_z, y + cy * up_y)
                if where in cells:
                    index = cells.index(where)
                    tile = rx[begin + index // 8]
                    shift = (128 - 16 * (index % 8)) % 128
                    tile = pltpu.roll(tile, shift, 1) if shift else tile
                    extra = tile if extra is None else extra + tile
            value = value + jnp.where(lane < 16, extra, 0.0)
            hw_ref[cell] = value
            split_store(HW, cell, value)

    hw_row = products(HW, XX, HW + 1)
    second = jnp.where(lane < 96, hw_row, pltpu.roll(w_row2_pad(w_row2), 32, 1))
    red2_ref[...] = finish(reduced(1, jnp.concatenate([w_row, second], 0)))


def w_row2_pad(row):
    return jnp.concatenate([row, jnp.zeros((row.shape[0], 128 - row.shape[1]), row.dtype)], 1)


def per_device(
    sizes,
    block_x, block_hx, block_p, block_hp, potential, projectors, coupling,
    atom_count, proj_count, offsets, extents,
):
    cols, cz, cy, cx = block_x.shape
    slots, nproj = projectors.shape[-3], projectors.shape[-2]
    nz, ny, nx = sizes
    own = cz * cy
    fz, fy = cz + BZ - 1, cy + BY - 1
    beta = masked_projectors(projectors, atom_count, proj_count, extents)[0, 0, 0]
    beta = beta.reshape(slots, nproj, BZ * BY, BX).transpose(0, 2, 1, 3)
    beta = beta.reshape(slots * BZ * BY * nproj, BX)
    beta = jnp.pad(beta, ((0, 0), (0, 128 - BX)))
    sym = (0.5 * (coupling + jnp.swapaxes(coupling, -1, -2))).reshape(-1)
    turned = [
        jnp.transpose(b, (1, 2, 0, 3)).reshape(own, cols, cx)
        for b in (block_x, block_hx, block_p, block_hp)
    ]
    groups = (("gz", "gy"), ("gx",)) if nz * ny <= 16 else (("gz",), ("gy",), ("gx",))
    size_of = dict(zip(AXES, sizes))
    totals = []
    for group in groups:
        total = 1
        for a in group:
            total *= size_of[a]
        totals.append(total)
    tile = (cols, 128)
    more_z, more_y = fz - cz, fy - cy
    packed = sum(
        tiles_of(zc * yc) for zc in (cz, more_z) for yc in (cy, more_y)
    )
    per_slot = BZ * BY * nproj
    scratch = [
        pltpu.VMEM((192, own * 128), BF16),
        pltpu.VMEM((3 * own,) + tile, F32),
        pltpu.VMEM((2, own) + tile, F32),
        pltpu.VMEM(((BZ - 1) * cy,) + tile, F32),
        pltpu.VMEM((tiles_of(own),) + tile, F32),
        pltpu.VMEM((tiles_of(own),) + tile, F32),
        pltpu.VMEM((4, tiles_of(own)) + tile, F32),
        pltpu.VMEM((tiles_of(own),) + tile, F32),
        pltpu.VMEM((fz * fy,) + tile, F32),
        pltpu.VMEM((fz * fy,) + tile, F32),
        pltpu.VMEM((own,) + tile, F32),
        pltpu.VMEM((slots * per_slot, 128), F32),
        pltpu.VMEM((slots * per_slot, 128), F32),
        pltpu.VMEM((slots * (BZ + 2) * (BY + 2), 2) + tile, F32),
        pltpu.VMEM((fz, fy) + tile, F32),
        pltpu.VMEM((fz, fy) + tile, F32),
        pltpu.VMEM((packed,) + tile, F32),
        pltpu.VMEM((more_z, cy) + tile, F32),
        pltpu.VMEM((cz, more_y) + tile, F32),
        pltpu.VMEM((more_z, more_y) + tile, F32),
        pltpu.VMEM((packed,) + tile, F32),
        pltpu.VMEM((8, 128), F32),
    ]
    scratch += [pltpu.VMEM((t, 2 * cols, 128), F32) for t in totals] * 2
    scratch += [
        pltpu.SemaphoreType.DMA((2 * sum(totals),)),
        pltpu.SemaphoreType.DMA((2 * sum(totals),)),
        pltpu.SemaphoreType.DMA((10,)),
        pltpu.SemaphoreType.DMA((10,)),
        pltpu.SemaphoreType.DMA((7,)),
        pltpu.SemaphoreType.DMA((7,)),
    ]
    vmem = pl.BlockSpec(memory_space=pltpu.VMEM)
    smem = pl.BlockSpec(memory_space=pltpu.SMEM)
    w, hw, red1, red2 = pl.pallas_call(
        functools.partial(kernel, sizes, groups, (cz, cy, cx, slots, nproj, cols)),
        out_shape=(
            jax.ShapeDtypeStruct((own,) + tile, F32),
            jax.ShapeDtypeStruct((own,) + tile, F32),
            jax.ShapeDtypeStruct((2 * cols, 128), F32),
            jax.ShapeDtypeStruct((2 * cols, 128), F32),
        ),
        in_specs=[smem, smem] + [vmem] * 6,
        out_specs=(vmem,) * 4,
        scratch_shapes=scratch,
        compiler_params=pltpu.CompilerParams(collective_id=0, has_side_effects=True),
    )(offsets.reshape(-1), sym, *turned, potential.reshape(own, 1, cx), beta)
    weight = 1.0 / (own * cx * nz * ny * nx)

    def block(rows, group):
        start = 32 * group
        return (rows[:, start : start + cols] + rows[:, start + cols : start + 2 * cols]) * weight

    x_row, p_row, w_row, hw_row = red1[:cols], red1[cols:], red2[:cols], red2[cols:]
    gram = jnp.block(
        [
            [block(x_row, 2), block(w_row, 2).T, block(x_row, 3)],
            [block(w_row, 2), block(hw_row, 3), block(w_row, 3)],
            [block(p_row, 2), block(w_row, 3).T, block(p_row, 3)],
        ]
    )
    rayleigh = jnp.block(
        [
            [block(x_row, 0).T, block(hw_row, 0).T, block(x_row, 1)],
            [block(w_row, 0), block(hw_row, 2).T, block(w_row, 1)],
            [block(p_row, 0), block(hw_row, 1).T, block(p_row, 1)],
        ]
    )
    w, hw = (jnp.transpose(b.reshape(cz, cy, cols, cx), (2, 0, 1, 3)) for b in (w, hw))
    return (w, hw, gram, rayleigh)


def solution(mesh):
    sizes = tuple(mesh.shape[a] for a in AXES)
    in_specs = (
        P(None, "gz", "gy", "gx"),
        P(None, "gz", "gy", "gx"),
        P(None, "gz", "gy", "gx"),
        P(None, "gz", "gy", "gx"),
        P("gz", "gy", "gx"),
        P("gz", "gy", "gx", None, None, None),
        P("gz", "gy", "gx", None, None, None),
        P("gz", "gy", "gx"),
        P("gz", "gy", "gx", None),
        P(None, "gz", "gy", "gx", None),
        P(None, "gz", "gy", "gx", None),
    )
    out_specs = (P(None, "gz", "gy", "gx"), P(None, "gz", "gy", "gx"), P(), P())
    return jax.shard_map(
        functools.partial(per_device, sizes),
        mesh=mesh, in_specs=in_specs, out_specs=out_specs, check_vma=False,
    )
```

```python
import functools

import jax
import jax.numpy as jnp
from jax import lax
from jax.experimental import pallas as pl
from jax.experimental.pallas import tpu as pltpu
from jax.sharding import PartitionSpec as P

BZ, BY, BX = 4, 4, 16
LAP_CENTER = -5369.0 / 1800.0
LAP_COEFFS = (12.0 / 7.0, -15.0 / 56.0, 10.0 / 189.0, -1.0 / 112.0, 2.0 / 1925.0, -1.0 / 16632.0)
MESH = pl.DeviceIdType.MESH
AXES = ("gz", "gy", "gx")
F32 = jnp.float32
BF16 = jnp.bfloat16
HP, HX, XX, PP, WW, HW = range(6)


def tiles_of(count):
    return -(-count // 8)


def kernel(
    sizes, groups, dims,
    off_ref, ext_ref, count_ref, proj_ref, d_ref, x_ref, hx_ref, p_ref, hp_ref, v_ref, beta_ref,
    w_ref, hw_ref, gram_ref, ray_ref, red1_ref,
    stack, zext, ybuf, zybuf, plow, phigh, xr, xl, frame, frame_x, halo_x,
    blo, bhi, pieces, nf, nh, spack, rz, ry, rzy, rx, wout,
    *rest,
):
    cz, cy, cx, slots, nproj, cols = dims
    nz, ny, nx = sizes
    n_red = len(groups)
    bufs = (rest[:n_red], rest[n_red : 2 * n_red])
    rest = rest[2 * n_red :]
    red_send, red_recv, halo_send, halo_recv, spill_send, spill_recv = rest
    zi, yi, xi = (lax.axis_index(a) for a in AXES)
    size_of = dict(zip(AXES, sizes))
    here = dict(zip(AXES, (zi, yi, xi)))
    fz, fy = cz + BZ - 1, cy + BY - 1
    own = cz * cy
    lane = lax.broadcasted_iota(jnp.int32, (cols, 128), 1)

    def neighbour(dz, dy, dx):
        step = dict(zip(AXES, (dz, dy, dx)))
        return {a: lax.rem(here[a] + step[a] + size_of[a], size_of[a]) for a in AXES}

    def member(group, offset):
        total = 1
        index = 0
        for a in group:
            total *= size_of[a]
            index = index * size_of[a] + here[a]
        target = lax.rem(index + offset, total)
        device = {}
        for a in reversed(group):
            device[a] = lax.rem(target, size_of[a])
            target = target // size_of[a]
        return {a: device.get(a, here[a]) for a in AXES}, index, total

    octant = [(1, 0, 0), (0, 1, 0), (1, 1, 0), (0, 0, 1), (1, 0, 1), (0, 1, 1), (1, 1, 1)]
    barrier = pltpu.get_barrier_semaphore()
    greeted = 0
    for group in groups:
        total = member(group, 0)[2]
        for offset in range(1, total):
            pl.semaphore_signal(
                barrier, inc=1, device_id=member(group, offset)[0], device_id_type=MESH
            )
            greeted += 1
    for dz, dy, dx in octant:
        for sign in (1, -1):
            pl.semaphore_signal(
                barrier, inc=1, device_id=neighbour(sign * dz, sign * dy, sign * dx),
                device_id_type=MESH,
            )
            greeted += 1

    def split_store(kind, cell, value):
        high = value.astype(BF16)
        low = (value - high.astype(F32)).astype(BF16)
        start = cell * 128 if isinstance(cell, int) else pl.multiple_of(cell * 128, 128)
        stack[kind * 32 : kind * 32 + 32, pl.ds(start, 128)] = jnp.concatenate([high, low], 0)

    @pl.loop(0, cz)
    def _(z):
        for y in range(cy):
            cell = z * cy + y
            split_store(HX, cell, hx_ref[cell])
            split_store(HP, cell, hp_ref[cell])
            split_store(XX, cell, x_ref[cell])
            split_store(PP, cell, p_ref[cell])

    def products(left, right_from, right_to, count=1):
        m = lax.dot_general(
            stack[left * 32 : (left + count) * 32, :],
            stack[right_from * 32 : right_to * 32, :],
            (((1,), (1,)), ((), ())),
            preferred_element_type=F32,
        )
        parts = [m[32 * i : 32 * i + cols] + m[32 * i + cols : 32 * i + 32] for i in range(count)]
        return parts if count > 1 else parts[0]

    def reduced(which, payload):
        base = which * sum(member(g, 0)[2] for g in groups)
        for phase, group in enumerate(groups):
            buf = bufs[which][phase]
            _, index, total = member(group, 0)
            buf[index] = payload
            if phase == 0 and which == 0:
                pl.semaphore_wait(barrier, greeted)
            copies = []
            for offset in range(1, total):
                copies.append(
                    pltpu.make_async_remote_copy(
                        src_ref=buf.at[index],
                        dst_ref=buf.at[index],
                        send_sem=red_send.at[base + offset],
                        recv_sem=red_recv.at[base + offset],
                        device_id=member(group, offset)[0],
                        device_id_type=MESH,
                    )
                )
                copies[-1].start()
            base += total
            yield None
            for copy in copies:
                copy.wait()
            payload = buf[0]
            for slot in range(1, total):
                payload = payload + buf[slot]
        yield payload

    def finish(steps):
        out = None
        for out in steps:
            pass
        return out

    hx_row, x_row, p_row = products(HX, HP, WW, 3)
    first = jnp.where((lane >= 32) & (lane < 64), pltpu.roll(hx_row, 96, 1), x_row)

    def paired(upper, lower):
        upper = upper + pltpu.roll(upper, 112, 1)
        lower = lower + pltpu.roll(lower, 112, 1)
        return jnp.where(lane % 32 < 16, upper, pltpu.roll(lower, 16, 1))

    reduction = reduced(0, paired(first, p_row))
    next(reduction)

    per_slot = BZ * BY * nproj
    lane_p = lax.broadcasted_iota(jnp.int32, (nproj, 128), 1)
    row_p = lax.broadcasted_iota(jnp.int32, (nproj, 128), 0)
    in_tile = 128 // BX
    for s in range(slots):
        ox = off_ref[2, s]
        along = lax.rem(lane_p - ox + 128, 128)
        along = jnp.where(row_p < proj_ref[0, s], along, 128)
        low_side = lane_p >= ox
        live = s < count_ref[0, 0]
        for a in range(BZ):
            for b in range(BY):
                used = live & (a < ext_ref[0, s]) & (b < ext_ref[1, s])
                limit = jnp.where(used, jnp.minimum(ext_ref[2, s], BX), 0)
                box = a * BY + b
                part = beta_ref[s, :, (box // in_tile) * 128 : (box // in_tile) * 128 + 128]
                part = pltpu.roll(part, lax.rem(ox + 128 - BX * (box % in_tile), 128), 1)
                part = jnp.where(along < limit, part, 0.0)
                row = s * per_slot + box * nproj
                blo[row : row + nproj, :] = jnp.where(low_side, part, 0.0)
                bhi[row : row + nproj, :] = jnp.where(low_side, 0.0, part)
    rim_y = BY + 2
    rim = (BZ + 2) * rim_y

    @pl.loop(0, slots)
    def _(s):
        for i in range(rim):
            if i < rim_y or i >= rim - rim_y or i % rim_y in (0, rim_y - 1):
                pieces[s * rim + i] = jnp.zeros(pieces.shape[1:], F32)

    sums1 = finish(reduction)
    red1_ref[...] = sums1
    matrix = jnp.concatenate([pltpu.roll(sums1, 64, 1), pltpu.roll(sums1, 96, 1)], 0)
    lane2 = lax.broadcasted_iota(jnp.int32, (2 * cols, 128), 1)
    matrix = jnp.where(lane2 < cols, matrix, 0.0)
    for k in range(cols):
        row = matrix[k : k + 1, :]
        column = matrix[:, k : k + 1] / matrix[k : k + 1, k : k + 1]
        matrix = jnp.where(lane2 == k, column, matrix - column * row)
    theta_t = matrix[cols:, :]
    theta_cols = [jnp.broadcast_to(theta_t[:, k : k + 1], (cols, 128)) for k in range(cols)]

    @pl.loop(0, cz)
    def _(z):
        for y in range(cy):
            cell = z * cy + y
            xs = x_ref[cell]
            value = hx_ref[cell]
            for k in range(cols):
                value = value - theta_cols[k] * xs[k : k + 1, :]
            vv = v_ref[z, y : y + 1, :]
            value = value / (1.0 + vv * vv)
            zext[cz + z, y] = value
            w_ref[cell] = value
            split_store(WW, cell, value)

    for q in range(tiles_of(own)):
        low = jnp.zeros((cols, 128), F32)
        high = low
        for j in range(min(8, own - 8 * q)):
            tile = zext[cz + (8 * q + j) // cy, (8 * q + j) % cy]
            keep = (lane >= 16 * j) & (lane < 16 * j + 16)
            low = jnp.where(keep, pltpu.roll(tile, 16 * j, 1) if j else tile, low)
            high = jnp.where(keep, pltpu.roll(tile, (16 * j + 16) % 128, 1) if j < 7 else tile, high)
        plow[q] = low
        phigh[q] = high

    two_y = ny == 2
    more_z, more_y = fz - cz, fy - cy
    z_tiles = tiles_of(more_z * cy)
    corner_tiles = tiles_of((more_z - 1) * cy + more_y)

    def some(ref, z, dz, y, dy):
        return ref.at[pl.ds(z, dz), pl.ds(y, dy)]

    def layers(target, base, z, dz, y, dy, where):
        return some(zext, cz + z, dz, y, dy), some(target, base + z, dz, y, dy), where

    early = [
        (some(zext, cz, more_z, 0, more_y), zybuf, (-1, -1, 0)),
        (plow.at[pl.ds(0, corner_tiles)], xr.at[3, pl.ds(0, corner_tiles)], (-1, -1, -1)),
        (plow, xr.at[2], (0, -1, -1)),
        (plow.at[pl.ds(0, z_tiles)], xr.at[1, pl.ds(0, z_tiles)], (-1, 0, -1)),
        (plow, xr.at[0], (0, 0, -1)),
        layers(ybuf.at[1], 0, 0, cz, 0, more_y, (0, -1, 0)),
        layers(zext, 2 * cz, 0, more_z, 0, cy, (-1, 0, 0)),
    ]
    late = [
        (phigh, xl, (0, 0, 1)),
        layers(ybuf.at[1], 0, 0, cz, more_y, cy - more_y, (0, -1, 0)),
        layers(zext, 2 * cz, more_z, cz - more_z, 0, cy, (-1, 0, 0)),
        layers(zext, 0, 0, cz, 0, cy, (1, 0, 0)),
    ]
    if not two_y:
        late.append(layers(ybuf.at[0], 0, 0, cz, 0, cy, (0, 1, 0)))

    def launch(sends, send_sem, recv_sem, first=0):
        copies = []
        for i, (source, target, where) in enumerate(sends, start=first):
            copies.append(
                pltpu.make_async_remote_copy(
                    src_ref=source,
                    dst_ref=target,
                    send_sem=send_sem.at[i],
                    recv_sem=recv_sem.at[i],
                    device_id=neighbour(*where),
                    device_id_type=MESH,
                )
            )
            copies[-1].start()
        return copies

    copies = launch(early, halo_send, halo_recv)
    late_copies = launch(late, halo_send, halo_recv, len(early))
    w_row = products(WW, HP, WW)
    w_row2 = products(WW, XX, HW)
    for copy in copies:
        copy.wait()

    below_y = 1 if two_y else 0
    for z in range(fz):
        for y in range(fy):
            up_z, up_y = z >= cz, y >= cy
            local = (z - cz * up_z) * cy + (y - cy * up_y)
            if up_z and up_y:
                tile = zybuf[z - cz, y - cy]
            elif up_z:
                tile = zext[cz + z, y]
            elif up_y:
                tile = ybuf[1, z, y - cy]
            else:
                tile = zext[cz + z, y]
            frame[z * fy + y] = tile
            shift = (128 - 16 * (local % 8)) % 128
            tile = xr[up_z + 2 * up_y, local // 8]
            tile = pltpu.roll(tile, shift, 1) if shift else tile
            frame_x[z * fy + y] = tile

    @pl.loop(0, slots)
    def _(s):
        oz, oy = off_ref[0, s], off_ref[1, s]
        sums = [jnp.zeros((cols, 128), F32) for _ in range(nproj)]
        for a in range(BZ):
            for b in range(BY):
                at = (oz + a) * fy + oy + b
                tile, tile_x = frame[at], frame_x[at]
                base = s * per_slot + (a * BY + b) * nproj
                for q in range(nproj):
                    sums[q] = sums[q] + tile * blo[pl.ds(base + q, 1), :]
                    sums[q] = sums[q] + jnp.where(
                        lane < 16, tile_x * bhi[pl.ds(base + q, 1), :], 0.0
                    )
        overlaps = [jnp.broadcast_to(jnp.sum(v, axis=1, keepdims=True), (cols, 128)) for v in sums]
        outs = []
        for p in range(nproj):
            value = overlaps[p] * d_ref[s, p, p]
            for q in range(nproj):
                if q != p:
                    value = value + overlaps[q] * (0.5 * (d_ref[s, p, q] + d_ref[s, q, p]))
            outs.append(value)
        for a in range(BZ):
            for b in range(BY):
                base = s * per_slot + (a * BY + b) * nproj
                low = outs[0] * blo[pl.ds(base, 1), :]
                high = outs[0] * bhi[pl.ds(base, 1), :]
                for p in range(1, nproj):
                    low = low + outs[p] * blo[pl.ds(base + p, 1), :]
                    high = high + outs[p] * bhi[pl.ds(base + p, 1), :]
                place = s * rim + (a + 1) * rim_y + b + 1
                pieces[place, 0] = low
                pieces[place, 1] = high

    @pl.loop(0, fz)
    def _(z):
        starts = []
        for s in range(slots):
            a = jnp.minimum(jnp.maximum(z - off_ref[0, s], -1), BZ) + 1
            starts.append(s * rim + a * rim_y)
        for y in range(fy):
            low = jnp.zeros((cols, 128), F32)
            high = low
            for s in range(slots):
                b = jnp.minimum(jnp.maximum(y - off_ref[1, s], -1), BY) + 1
                low = low + pieces[starts[s] + b, 0]
                high = high + pieces[starts[s] + b, 1]
            nf[z, y] = low
            nh[z, y] = high

    spans = []
    filled = 0
    for up_z in (0, 1):
        for up_y in (0, 1):
            cells = [
                (z, y)
                for z in (range(cz, fz) if up_z else range(cz))
                for y in (range(cy, fy) if up_y else range(cy))
            ]
            spans.append((filled, up_z, up_y, cells))
            for q in range(tiles_of(len(cells))):
                tile = jnp.zeros((cols, 128), F32)
                for j, (z, y) in enumerate(cells[8 * q : 8 * q + 8]):
                    keep = (lane >= 16 * j) & (lane < 16 * j + 16)
                    value = nh[z, y]
                    tile = jnp.where(keep, pltpu.roll(value, 16 * j, 1) if j else value, tile)
                spack[filled + q] = tile
            filled += tiles_of(len(cells))
    sends = [
        (nf.at[pl.ds(cz, more_z), pl.ds(0, cy)], rz, (1, 0, 0)),
        (nf.at[pl.ds(0, cz), pl.ds(cy, more_y)], ry, (0, 1, 0)),
        (nf.at[pl.ds(cz, more_z), pl.ds(cy, more_y)], rzy, (1, 1, 0)),
    ]
    for begin, up_z, up_y, cells in spans:
        part = pl.ds(begin, tiles_of(len(cells)))
        sends.append((spack.at[part], rx.at[part], (up_z, up_y, 1)))
    copies = launch(sends, spill_send, spill_recv)

    for copy in late_copies:
        copy.wait()
    for cell in range(own):
        turn = (112 - 16 * (cell % 8)) % 128
        left = xl[cell // 8]
        left = pltpu.roll(left, turn, 1) if turn else left
        halo_x[cell] = jnp.where(lane < 64, frame_x[cell // cy * fy + cell % cy], left)

    @pl.loop(0, cz)
    def _(z):
        for y in range(cy):
            cell = z * cy + y
            centre = zext[cz + z, y]
            edge = halo_x[cell]
            vv = v_ref[z, y : y + 1, :]
            total = centre * (vv - 1.5 * LAP_CENTER)
            for k, weight in enumerate(LAP_COEFFS, start=1):
                beside = zext[cz + z + k, y] + zext[cz + z - k, y]
                for target in (y + k, y - k):
                    if target >= cy:
                        beside = beside + ybuf[1, z, target - cy]
                    elif target < 0:
                        beside = beside + ybuf[below_y, z, target + cy]
                    else:
                        beside = beside + zext[cz + z, target]
                beside = beside + pltpu.roll(jnp.where(lane < k, edge, centre), 128 - k, 1)
                beside = beside + pltpu.roll(jnp.where(lane >= 128 - k, edge, centre), k, 1)
                total = total - 0.5 * weight * beside
            hw_ref[cell] = total + nf[z, y]

    for copy in copies:
        copy.wait()
    for z in range(cz):
        for y in range(cy):
            cell = z * cy + y
            value = hw_ref[cell]
            if z < more_z:
                value = value + rz[z, y]
            if y < more_y:
                value = value + ry[z, y]
            if z < more_z and y < more_y:
                value = value + rzy[z, y]
            extra = None
            for begin, up_z, up_y, cells in spans:
                where = (z + cz * up_z, y + cy * up_y)
                if where in cells:
                    index = cells.index(where)
                    tile = rx[begin + index // 8]
                    shift = (128 - 16 * (index % 8)) % 128
                    tile = pltpu.roll(tile, shift, 1) if shift else tile
                    extra = tile if extra is None else extra + tile
            value = value + jnp.where(lane < 16, extra, 0.0)
            hw_ref[cell] = value
            split_store(HW, cell, value)

    hw_row = products(HW, XX, HW + 1)
    second = jnp.where(lane < 96, hw_row, pltpu.roll(w_row2_pad(w_row2), 32, 1))
    sums2 = finish(reduced(1, paired(w_row, second)))
    weight = 1.0 / (own * cx * nz * ny * nx)
    sums1 = red1_ref[...]
    rows = jnp.concatenate([sums1, pltpu.roll(sums1, 112, 1), sums2, pltpu.roll(sums2, 112, 1)], 0)
    rows = rows * weight
    turned = jnp.transpose(jnp.concatenate([rows, jnp.zeros_like(rows)], 0))

    def direct(row, group, target):
        return rows[16 * row : 16 * row + 16, :], 32 * group, target

    def flipped(row, group, target):
        return turned[32 * group : 32 * group + 16, :], 16 * row, target

    def laid(parts):
        total = None
        for tile, begin, target in parts:
            shift = (16 * target - begin) % 128
            tile = pltpu.roll(tile, shift, 1) if shift else tile
            tile = jnp.where((lane >= 16 * target) & (lane < 16 * target + 16), tile, 0.0)
            total = tile if total is None else total + tile
        return total

    gram = [
        [direct(0, 2, 0), flipped(2, 2, 1), direct(0, 3, 2)],
        [direct(2, 2, 0), direct(3, 3, 1), direct(2, 3, 2)],
        [direct(1, 2, 0), flipped(2, 3, 1), direct(1, 3, 2)],
    ]
    rayleigh = [
        [flipped(0, 1, 0), flipped(3, 0, 1), direct(0, 0, 2)],
        [direct(2, 1, 0), flipped(3, 2, 1), direct(2, 0, 2)],
        [direct(1, 1, 0), flipped(3, 1, 1), direct(1, 0, 2)],
    ]
    for i in range(3):
        gram_ref[16 * i : 16 * i + 16, :] = laid(gram[i])[:, :48]
        ray_ref[16 * i : 16 * i + 16, :] = laid(rayleigh[i])[:, :48]


def w_row2_pad(row):
    return jnp.concatenate([row, jnp.zeros((row.shape[0], 128 - row.shape[1]), row.dtype)], 1)


def per_device(
    sizes,
    block_x, block_hx, block_p, block_hp, potential, projectors, coupling,
    atom_count, proj_count, offsets, extents,
):
    cols, cz, cy, cx = block_x.shape
    slots, nproj = projectors.shape[-3], projectors.shape[-2]
    nz, ny, nx = sizes
    own = cz * cy
    fz, fy = cz + BZ - 1, cy + BY - 1
    turned = [
        jnp.transpose(b, (1, 2, 0, 3)).reshape(own, cols, cx)
        for b in (block_x, block_hx, block_p, block_hp)
    ]
    groups = (("gz", "gy"), ("gx",)) if nz * ny <= 16 else (("gz",), ("gy",), ("gx",))
    size_of = dict(zip(AXES, sizes))
    totals = []
    for group in groups:
        total = 1
        for a in group:
            total *= size_of[a]
        totals.append(total)
    tile = (cols, 128)
    more_z, more_y = fz - cz, fy - cy
    packed = sum(
        tiles_of(zc * yc) for zc in (cz, more_z) for yc in (cy, more_y)
    )
    per_slot = BZ * BY * nproj
    scratch = [
        pltpu.VMEM((cols, 128), F32),
        pltpu.VMEM((192, own * 128), BF16),
        pltpu.VMEM((3 * cz, cy) + tile, F32),
        pltpu.VMEM((2, cz, cy) + tile, F32),
        pltpu.VMEM((BZ - 1, BY - 1) + tile, F32),
        pltpu.VMEM((tiles_of(own),) + tile, F32),
        pltpu.VMEM((tiles_of(own),) + tile, F32),
        pltpu.VMEM((4, tiles_of(own)) + tile, F32),
        pltpu.VMEM((tiles_of(own),) + tile, F32),
        pltpu.VMEM((fz * fy,) + tile, F32),
        pltpu.VMEM((fz * fy,) + tile, F32),
        pltpu.VMEM((own,) + tile, F32),
        pltpu.VMEM((slots * per_slot, 128), F32),
        pltpu.VMEM((slots * per_slot, 128), F32),
        pltpu.VMEM((slots * (BZ + 2) * (BY + 2), 2) + tile, F32),
        pltpu.VMEM((fz, fy) + tile, F32),
        pltpu.VMEM((fz, fy) + tile, F32),
        pltpu.VMEM((packed,) + tile, F32),
        pltpu.VMEM((more_z, cy) + tile, F32),
        pltpu.VMEM((cz, more_y) + tile, F32),
        pltpu.VMEM((more_z, more_y) + tile, F32),
        pltpu.VMEM((packed,) + tile, F32),
        pltpu.VMEM((8, 128), F32),
    ]
    scratch += [pltpu.VMEM((t, cols, 128), F32) for t in totals] * 2
    scratch += [
        pltpu.SemaphoreType.DMA((2 * sum(totals),)),
        pltpu.SemaphoreType.DMA((2 * sum(totals),)),
        pltpu.SemaphoreType.DMA((12,)),
        pltpu.SemaphoreType.DMA((12,)),
        pltpu.SemaphoreType.DMA((7,)),
        pltpu.SemaphoreType.DMA((7,)),
    ]
    vmem = pl.BlockSpec(memory_space=pltpu.VMEM)
    smem = pl.BlockSpec(memory_space=pltpu.SMEM)
    w, hw, gram, rayleigh = pl.pallas_call(
        functools.partial(kernel, sizes, groups, (cz, cy, cx, slots, nproj, cols)),
        out_shape=(
            jax.ShapeDtypeStruct((own,) + tile, F32),
            jax.ShapeDtypeStruct((own,) + tile, F32),
            jax.ShapeDtypeStruct((3 * cols, 3 * cols), F32),
            jax.ShapeDtypeStruct((3 * cols, 3 * cols), F32),
        ),
        in_specs=[smem] * 5 + [vmem] * 6,
        out_specs=(vmem,) * 4,
        scratch_shapes=scratch,
        compiler_params=pltpu.CompilerParams(collective_id=0, has_side_effects=True),
    )(
        offsets[:, 0, 0, 0], extents[:, 0, 0, 0], atom_count[0], proj_count[0, 0], coupling[0, 0, 0],
        *turned, potential, projectors[0, 0, 0],
    )
    w, hw = (jnp.transpose(b.reshape(cz, cy, cols, cx), (2, 0, 1, 3)) for b in (w, hw))
    return (w, hw, gram, rayleigh)


def solution(mesh):
    sizes = tuple(mesh.shape[a] for a in AXES)
    in_specs = (
        P(None, "gz", "gy", "gx"),
        P(None, "gz", "gy", "gx"),
        P(None, "gz", "gy", "gx"),
        P(None, "gz", "gy", "gx"),
        P("gz", "gy", "gx"),
        P("gz", "gy", "gx", None, None, None),
        P("gz", "gy", "gx", None, None, None),
        P("gz", "gy", "gx"),
        P("gz", "gy", "gx", None),
        P(None, "gz", "gy", "gx", None),
        P(None, "gz", "gy", "gx", None),
    )
    out_specs = (P(None, "gz", "gy", "gx"), P(None, "gz", "gy", "gx"), P(), P())
    return jax.shard_map(
        functools.partial(per_device, sizes),
        mesh=mesh, in_specs=in_specs, out_specs=out_specs, check_vma=False,
    )
```

```python
import functools

import jax
import jax.numpy as jnp
from jax import lax
from jax.experimental import pallas as pl
from jax.experimental.pallas import tpu as pltpu
from jax.sharding import PartitionSpec as P

BZ, BY, BX = 4, 4, 16
LAP_CENTER = -5369.0 / 1800.0
LAP_COEFFS = (12.0 / 7.0, -15.0 / 56.0, 10.0 / 189.0, -1.0 / 112.0, 2.0 / 1925.0, -1.0 / 16632.0)
MESH = pl.DeviceIdType.MESH
AXES = ("gz", "gy", "gx")
F32 = jnp.float32
BF16 = jnp.bfloat16
HP, HX, XX, PP, WW, HW = range(6)


def tiles_of(count):
    return -(-count // 8)


def kernel(
    sizes, groups, dims,
    off_ref, ext_ref, count_ref, proj_ref, d_ref, x_in, hx_in, p_in, hp_in, v_ref, beta_ref,
    w_ref, hw_ref, gram_ref, ray_ref, red1_ref,
    stack, zext, ybuf, zybuf, plow, phigh, xr, xl, frame, frame_x, halo_x,
    blo, bhi, pieces, nf, nh, spack, rz, ry, rzy, rx, wout,
    *rest,
):
    cz, cy, cx, slots, nproj, cols = dims
    nz, ny, nx = sizes
    n_red = len(groups)
    bufs = (rest[:n_red], rest[n_red : 2 * n_red])
    rest = rest[2 * n_red :]
    red_send, red_recv, halo_send, halo_recv, spill_send, spill_recv = rest[:6]
    load_sem, x_ref, hx_ref, p_ref, hp_ref = rest[6:]
    loads = []
    for i, (source, target) in enumerate(
        ((x_in, x_ref), (hx_in, hx_ref), (p_in, p_ref), (hp_in, hp_ref))
    ):
        loads.append(pltpu.make_async_copy(source, target, load_sem.at[i]))
        loads[-1].start()
    zi, yi, xi = (lax.axis_index(a) for a in AXES)
    size_of = dict(zip(AXES, sizes))
    here = dict(zip(AXES, (zi, yi, xi)))
    fz, fy = cz + BZ - 1, cy + BY - 1
    own = cz * cy
    lane = lax.broadcasted_iota(jnp.int32, (cols, 128), 1)

    def neighbour(dz, dy, dx):
        step = dict(zip(AXES, (dz, dy, dx)))
        return {a: lax.rem(here[a] + step[a] + size_of[a], size_of[a]) for a in AXES}

    def member(group, offset):
        total = 1
        index = 0
        for a in group:
            total *= size_of[a]
            index = index * size_of[a] + here[a]
        target = lax.rem(index + offset, total)
        device = {}
        for a in reversed(group):
            device[a] = lax.rem(target, size_of[a])
            target = target // size_of[a]
        return {a: device.get(a, here[a]) for a in AXES}, index, total

    octant = [(1, 0, 0), (0, 1, 0), (1, 1, 0), (0, 0, 1), (1, 0, 1), (0, 1, 1), (1, 1, 1)]
    barrier = pltpu.get_barrier_semaphore()
    greeted = 0
    for group in groups:
        total = member(group, 0)[2]
        for offset in range(1, total):
            pl.semaphore_signal(
                barrier, inc=1, device_id=member(group, offset)[0], device_id_type=MESH
            )
            greeted += 1
    for dz, dy, dx in octant:
        for sign in (1, -1):
            pl.semaphore_signal(
                barrier, inc=1, device_id=neighbour(sign * dz, sign * dy, sign * dx),
                device_id_type=MESH,
            )
            greeted += 1

    def split_store(kind, cell, value):
        high = value.astype(BF16)
        low = (value - high.astype(F32)).astype(BF16)
        start = cell * 128 if isinstance(cell, int) else pl.multiple_of(cell * 128, 128)
        stack[kind * 32 : kind * 32 + 32, pl.ds(start, 128)] = jnp.concatenate([high, low], 0)

    for load in loads:
        load.wait()

    @pl.loop(0, cz)
    def _(z):
        for y in range(cy):
            cell = z * cy + y
            split_store(HX, cell, hx_ref[cell])
            split_store(HP, cell, hp_ref[cell])
            split_store(XX, cell, x_ref[cell])
            split_store(PP, cell, p_ref[cell])

    def products(left, right_from, right_to, count=1):
        m = lax.dot_general(
            stack[left * 32 : (left + count) * 32, :],
            stack[right_from * 32 : right_to * 32, :],
            (((1,), (1,)), ((), ())),
            preferred_element_type=F32,
        )
        parts = [m[32 * i : 32 * i + cols] + m[32 * i + cols : 32 * i + 32] for i in range(count)]
        return parts if count > 1 else parts[0]

    def reduced(which, payload):
        base = which * sum(member(g, 0)[2] for g in groups)
        for phase, group in enumerate(groups):
            buf = bufs[which][phase]
            _, index, total = member(group, 0)
            buf[index] = payload
            if phase == 0 and which == 0:
                pl.semaphore_wait(barrier, greeted)
            copies = []
            for offset in range(1, total):
                copies.append(
                    pltpu.make_async_remote_copy(
                        src_ref=buf.at[index],
                        dst_ref=buf.at[index],
                        send_sem=red_send.at[base + offset],
                        recv_sem=red_recv.at[base + offset],
                        device_id=member(group, offset)[0],
                        device_id_type=MESH,
                    )
                )
                copies[-1].start()
            base += total
            yield None
            for copy in copies:
                copy.wait()
            payload = buf[0]
            for slot in range(1, total):
                payload = payload + buf[slot]
        yield payload

    def finish(steps):
        out = None
        for out in steps:
            pass
        return out

    hx_row, x_row, p_row = products(HX, HP, WW, 3)
    first = jnp.where((lane >= 32) & (lane < 64), pltpu.roll(hx_row, 96, 1), x_row)

    def paired(upper, lower):
        upper = upper + pltpu.roll(upper, 112, 1)
        lower = lower + pltpu.roll(lower, 112, 1)
        return jnp.where(lane % 32 < 16, upper, pltpu.roll(lower, 16, 1))

    reduction = reduced(0, paired(first, p_row))
    next(reduction)

    per_slot = BZ * BY * nproj
    lane_p = lax.broadcasted_iota(jnp.int32, (nproj, 128), 1)
    row_p = lax.broadcasted_iota(jnp.int32, (nproj, 128), 0)
    in_tile = 128 // BX
    for s in range(slots):
        ox = off_ref[2, s]
        along = lax.rem(lane_p - ox + 128, 128)
        along = jnp.where(row_p < proj_ref[0, s], along, 128)
        low_side = lane_p >= ox
        live = s < count_ref[0, 0]
        for a in range(BZ):
            for b in range(BY):
                used = live & (a < ext_ref[0, s]) & (b < ext_ref[1, s])
                limit = jnp.where(used, jnp.minimum(ext_ref[2, s], BX), 0)
                box = a * BY + b
                part = beta_ref[s, :, (box // in_tile) * 128 : (box // in_tile) * 128 + 128]
                part = pltpu.roll(part, lax.rem(ox + 128 - BX * (box % in_tile), 128), 1)
                part = jnp.where(along < limit, part, 0.0)
                row = s * per_slot + box * nproj
                blo[row : row + nproj, :] = jnp.where(low_side, part, 0.0)
                bhi[row : row + nproj, :] = jnp.where(low_side, 0.0, part)
    rim_y = BY + 2
    rim = (BZ + 2) * rim_y

    @pl.loop(0, slots)
    def _(s):
        for i in range(rim):
            if i < rim_y or i >= rim - rim_y or i % rim_y in (0, rim_y - 1):
                pieces[s * rim + i] = jnp.zeros(pieces.shape[1:], F32)

    sums1 = finish(reduction)
    red1_ref[...] = sums1
    matrix = jnp.concatenate([pltpu.roll(sums1, 64, 1), pltpu.roll(sums1, 96, 1)], 0)
    lane2 = lax.broadcasted_iota(jnp.int32, (2 * cols, 128), 1)
    matrix = jnp.where(lane2 < cols, matrix, 0.0)
    for k in range(0, cols, 2):
        row0, row1 = matrix[k : k + 1, :], matrix[k + 1 : k + 2, :]
        col0, col1 = matrix[:, k : k + 1], matrix[:, k + 1 : k + 2]
        a, b = matrix[k : k + 1, k : k + 1], matrix[k : k + 1, k + 1 : k + 2]
        c, d = matrix[k + 1 : k + 2, k : k + 1], matrix[k + 1 : k + 2, k + 1 : k + 2]
        ratio = c / a
        schur = d - ratio * b
        new1 = (col1 - col0 * (b / a)) / schur
        new0 = col0 / a - new1 * ratio
        rest_of = matrix - new0 * row0 - new1 * row1
        matrix = jnp.where(lane2 == k, new0, jnp.where(lane2 == k + 1, new1, rest_of))
    theta_t = matrix[cols:, :]
    theta_cols = [jnp.broadcast_to(theta_t[:, k : k + 1], (cols, 128)) for k in range(cols)]

    @pl.loop(0, cz)
    def _(z):
        for y in range(cy):
            cell = z * cy + y
            xs = x_ref[cell]
            value = hx_ref[cell]
            for k in range(cols):
                value = value - theta_cols[k] * xs[k : k + 1, :]
            vv = v_ref[z, y : y + 1, :]
            value = value / (1.0 + vv * vv)
            zext[cz + z, y] = value
            w_ref[cell] = value
            split_store(WW, cell, value)

    for q in range(tiles_of(own)):
        low = jnp.zeros((cols, 128), F32)
        high = low
        for j in range(min(8, own - 8 * q)):
            tile = zext[cz + (8 * q + j) // cy, (8 * q + j) % cy]
            keep = (lane >= 16 * j) & (lane < 16 * j + 16)
            low = jnp.where(keep, pltpu.roll(tile, 16 * j, 1) if j else tile, low)
            high = jnp.where(keep, pltpu.roll(tile, (16 * j + 16) % 128, 1) if j < 7 else tile, high)
        plow[q] = low
        phigh[q] = high

    two_y = ny == 2
    more_z, more_y = fz - cz, fy - cy
    z_tiles = tiles_of(more_z * cy)
    corner_tiles = tiles_of((more_z - 1) * cy + more_y)

    def some(ref, z, dz, y, dy):
        return ref.at[pl.ds(z, dz), pl.ds(y, dy)]

    def layers(target, base, z, dz, y, dy, where):
        return some(zext, cz + z, dz, y, dy), some(target, base + z, dz, y, dy), where

    early = [
        (some(zext, cz, more_z, 0, more_y), zybuf, (-1, -1, 0)),
        (plow.at[pl.ds(0, corner_tiles)], xr.at[3, pl.ds(0, corner_tiles)], (-1, -1, -1)),
        (plow, xr.at[2], (0, -1, -1)),
        (plow.at[pl.ds(0, z_tiles)], xr.at[1, pl.ds(0, z_tiles)], (-1, 0, -1)),
        (plow, xr.at[0], (0, 0, -1)),
        layers(ybuf.at[1], 0, 0, cz, 0, more_y, (0, -1, 0)),
        layers(zext, 2 * cz, 0, more_z, 0, cy, (-1, 0, 0)),
    ]
    late = [
        (phigh, xl, (0, 0, 1)),
        layers(ybuf.at[1], 0, 0, cz, more_y, cy - more_y, (0, -1, 0)),
        layers(zext, 2 * cz, more_z, cz - more_z, 0, cy, (-1, 0, 0)),
        layers(zext, 0, 0, cz, 0, cy, (1, 0, 0)),
    ]
    if not two_y:
        late.append(layers(ybuf.at[0], 0, 0, cz, 0, cy, (0, 1, 0)))

    def launch(sends, send_sem, recv_sem, first=0):
        copies = []
        for i, (source, target, where) in enumerate(sends, start=first):
            copies.append(
                pltpu.make_async_remote_copy(
                    src_ref=source,
                    dst_ref=target,
                    send_sem=send_sem.at[i],
                    recv_sem=recv_sem.at[i],
                    device_id=neighbour(*where),
                    device_id_type=MESH,
                )
            )
            copies[-1].start()
        return copies

    copies = launch(early, halo_send, halo_recv)
    late_copies = launch(late, halo_send, halo_recv, len(early))
    w_row = products(WW, HP, WW)
    w_row2 = products(WW, XX, HW)
    for copy in copies:
        copy.wait()

    below_y = 1 if two_y else 0
    for z in range(fz):
        for y in range(fy):
            up_z, up_y = z >= cz, y >= cy
            local = (z - cz * up_z) * cy + (y - cy * up_y)
            if up_z and up_y:
                tile = zybuf[z - cz, y - cy]
            elif up_z:
                tile = zext[cz + z, y]
            elif up_y:
                tile = ybuf[1, z, y - cy]
            else:
                tile = zext[cz + z, y]
            frame[z * fy + y] = tile
            shift = (128 - 16 * (local % 8)) % 128
            tile = xr[up_z + 2 * up_y, local // 8]
            tile = pltpu.roll(tile, shift, 1) if shift else tile
            frame_x[z * fy + y] = tile

    @pl.loop(0, slots)
    def _(s):
        oz, oy = off_ref[0, s], off_ref[1, s]
        sums = [jnp.zeros((cols, 128), F32) for _ in range(nproj)]
        for a in range(BZ):
            for b in range(BY):
                at = (oz + a) * fy + oy + b
                tile, tile_x = frame[at], frame_x[at]
                base = s * per_slot + (a * BY + b) * nproj
                for q in range(nproj):
                    sums[q] = sums[q] + tile * blo[pl.ds(base + q, 1), :]
                    sums[q] = sums[q] + jnp.where(
                        lane < 16, tile_x * bhi[pl.ds(base + q, 1), :], 0.0
                    )
        overlaps = [jnp.broadcast_to(jnp.sum(v, axis=1, keepdims=True), (cols, 128)) for v in sums]
        outs = []
        dm = d_ref[s]
        for p in range(nproj):
            value = overlaps[p] * dm[p : p + 1, p : p + 1]
            for q in range(nproj):
                if q != p:
                    value = value + overlaps[q] * (0.5 * (dm[p : p + 1, q : q + 1] + dm[q : q + 1, p : p + 1]))
            outs.append(value)
        for a in range(BZ):
            for b in range(BY):
                base = s * per_slot + (a * BY + b) * nproj
                low = outs[0] * blo[pl.ds(base, 1), :]
                high = outs[0] * bhi[pl.ds(base, 1), :]
                for p in range(1, nproj):
                    low = low + outs[p] * blo[pl.ds(base + p, 1), :]
                    high = high + outs[p] * bhi[pl.ds(base + p, 1), :]
                place = s * rim + (a + 1) * rim_y + b + 1
                pieces[place, 0] = low
                pieces[place, 1] = high

    @pl.loop(0, fz)
    def _(z):
        starts = []
        for s in range(slots):
            a = jnp.minimum(jnp.maximum(z - off_ref[0, s], -1), BZ) + 1
            starts.append(s * rim + a * rim_y)
        for y in range(fy):
            low = jnp.zeros((cols, 128), F32)
            high = low
            for s in range(slots):
                b = jnp.minimum(jnp.maximum(y - off_ref[1, s], -1), BY) + 1
                low = low + pieces[starts[s] + b, 0]
                high = high + pieces[starts[s] + b, 1]
            nf[z, y] = low
            nh[z, y] = high

    spans = []
    filled = 0
    for up_z in (0, 1):
        for up_y in (0, 1):
            cells = [
                (z, y)
                for z in (range(cz, fz) if up_z else range(cz))
                for y in (range(cy, fy) if up_y else range(cy))
            ]
            spans.append((filled, up_z, up_y, cells))
            for q in range(tiles_of(len(cells))):
                tile = jnp.zeros((cols, 128), F32)
                for j, (z, y) in enumerate(cells[8 * q : 8 * q + 8]):
                    keep = (lane >= 16 * j) & (lane < 16 * j + 16)
                    value = nh[z, y]
                    tile = jnp.where(keep, pltpu.roll(value, 16 * j, 1) if j else value, tile)
                spack[filled + q] = tile
            filled += tiles_of(len(cells))
    sends = [
        (nf.at[pl.ds(cz, more_z), pl.ds(0, cy)], rz, (1, 0, 0)),
        (nf.at[pl.ds(0, cz), pl.ds(cy, more_y)], ry, (0, 1, 0)),
        (nf.at[pl.ds(cz, more_z), pl.ds(cy, more_y)], rzy, (1, 1, 0)),
    ]
    for begin, up_z, up_y, cells in spans:
        part = pl.ds(begin, tiles_of(len(cells)))
        sends.append((spack.at[part], rx.at[part], (up_z, up_y, 1)))
    copies = launch(sends, spill_send, spill_recv)

    for copy in late_copies:
        copy.wait()
    for cell in range(own):
        turn = (112 - 16 * (cell % 8)) % 128
        left = xl[cell // 8]
        left = pltpu.roll(left, turn, 1) if turn else left
        halo_x[cell] = jnp.where(lane < 64, frame_x[cell // cy * fy + cell % cy], left)

    @pl.loop(0, cz)
    def _(z):
        for y in range(cy):
            cell = z * cy + y
            centre = zext[cz + z, y]
            edge = halo_x[cell]
            vv = v_ref[z, y : y + 1, :]
            total = centre * (vv - 1.5 * LAP_CENTER)
            for k, weight in enumerate(LAP_COEFFS, start=1):
                beside = zext[cz + z + k, y] + zext[cz + z - k, y]
                for target in (y + k, y - k):
                    if target >= cy:
                        beside = beside + ybuf[1, z, target - cy]
                    elif target < 0:
                        beside = beside + ybuf[below_y, z, target + cy]
                    else:
                        beside = beside + zext[cz + z, target]
                beside = beside + pltpu.roll(jnp.where(lane < k, edge, centre), 128 - k, 1)
                beside = beside + pltpu.roll(jnp.where(lane >= 128 - k, edge, centre), k, 1)
                total = total - 0.5 * weight * beside
            hw_ref[cell] = total + nf[z, y]

    for copy in copies:
        copy.wait()
    for z in range(cz):
        for y in range(cy):
            cell = z * cy + y
            value = hw_ref[cell]
            if z < more_z:
                value = value + rz[z, y]
            if y < more_y:
                value = value + ry[z, y]
            if z < more_z and y < more_y:
                value = value + rzy[z, y]
            extra = None
            for begin, up_z, up_y, cells in spans:
                where = (z + cz * up_z, y + cy * up_y)
                if where in cells:
                    index = cells.index(where)
                    tile = rx[begin + index // 8]
                    shift = (128 - 16 * (index % 8)) % 128
                    tile = pltpu.roll(tile, shift, 1) if shift else tile
                    extra = tile if extra is None else extra + tile
            value = value + jnp.where(lane < 16, extra, 0.0)
            hw_ref[cell] = value
            split_store(HW, cell, value)

    hw_row = products(HW, XX, HW + 1)
    second = jnp.where(lane < 96, hw_row, pltpu.roll(w_row2_pad(w_row2), 32, 1))
    sums2 = finish(reduced(1, paired(w_row, second)))
    weight = 1.0 / (own * cx * nz * ny * nx)
    sums1 = red1_ref[...]
    rows = jnp.concatenate([sums1, pltpu.roll(sums1, 112, 1), sums2, pltpu.roll(sums2, 112, 1)], 0)
    rows = rows * weight
    turned = jnp.transpose(jnp.concatenate([rows, jnp.zeros_like(rows)], 0))

    def direct(row, group, target):
        return rows[16 * row : 16 * row + 16, :], 32 * group, target

    def flipped(row, group, target):
        return turned[32 * group : 32 * group + 16, :], 16 * row, target

    def laid(parts):
        total = None
        for tile, begin, target in parts:
            shift = (16 * target - begin) % 128
            tile = pltpu.roll(tile, shift, 1) if shift else tile
            tile = jnp.where((lane >= 16 * target) & (lane < 16 * target + 16), tile, 0.0)
            total = tile if total is None else total + tile
        return total

    gram = [
        [direct(0, 2, 0), flipped(2, 2, 1), direct(0, 3, 2)],
        [direct(2, 2, 0), direct(3, 3, 1), direct(2, 3, 2)],
        [direct(1, 2, 0), flipped(2, 3, 1), direct(1, 3, 2)],
    ]
    rayleigh = [
        [flipped(0, 1, 0), flipped(3, 0, 1), direct(0, 0, 2)],
        [direct(2, 1, 0), flipped(3, 2, 1), direct(2, 0, 2)],
        [direct(1, 1, 0), flipped(3, 1, 1), direct(1, 0, 2)],
    ]
    for i in range(3):
        gram_ref[16 * i : 16 * i + 16, :] = laid(gram[i])[:, :48]
        ray_ref[16 * i : 16 * i + 16, :] = laid(rayleigh[i])[:, :48]


def put_out(*refs):
    half = len(refs) // 2
    for source, target in zip(refs[:half], refs[half:]):
        target[...] = source[...]


def w_row2_pad(row):
    return jnp.concatenate([row, jnp.zeros((row.shape[0], 128 - row.shape[1]), row.dtype)], 1)


def per_device(
    sizes,
    block_x, block_hx, block_p, block_hp, potential, projectors, coupling,
    atom_count, proj_count, offsets, extents,
):
    cols, cz, cy, cx = block_x.shape
    slots, nproj = projectors.shape[-3], projectors.shape[-2]
    nz, ny, nx = sizes
    own = cz * cy
    fz, fy = cz + BZ - 1, cy + BY - 1
    turned = [
        jnp.transpose(b, (1, 2, 0, 3)).reshape(own, cols, cx)
        for b in (block_x, block_hx, block_p, block_hp)
    ]
    groups = (("gz", "gy"), ("gx",)) if nz * ny <= 16 else (("gz",), ("gy",), ("gx",))
    size_of = dict(zip(AXES, sizes))
    totals = []
    for group in groups:
        total = 1
        for a in group:
            total *= size_of[a]
        totals.append(total)
    tile = (cols, 128)
    more_z, more_y = fz - cz, fy - cy
    packed = sum(
        tiles_of(zc * yc) for zc in (cz, more_z) for yc in (cy, more_y)
    )
    per_slot = BZ * BY * nproj
    scratch = [
        pltpu.VMEM((cols, 128), F32),
        pltpu.VMEM((192, own * 128), BF16),
        pltpu.VMEM((3 * cz, cy) + tile, F32),
        pltpu.VMEM((2, cz, cy) + tile, F32),
        pltpu.VMEM((BZ - 1, BY - 1) + tile, F32),
        pltpu.VMEM((tiles_of(own),) + tile, F32),
        pltpu.VMEM((tiles_of(own),) + tile, F32),
        pltpu.VMEM((4, tiles_of(own)) + tile, F32),
        pltpu.VMEM((tiles_of(own),) + tile, F32),
        pltpu.VMEM((fz * fy,) + tile, F32),
        pltpu.VMEM((fz * fy,) + tile, F32),
        pltpu.VMEM((own,) + tile, F32),
        pltpu.VMEM((slots * per_slot, 128), F32),
        pltpu.VMEM((slots * per_slot, 128), F32),
        pltpu.VMEM((slots * (BZ + 2) * (BY + 2), 2) + tile, F32),
        pltpu.VMEM((fz, fy) + tile, F32),
        pltpu.VMEM((fz, fy) + tile, F32),
        pltpu.VMEM((packed,) + tile, F32),
        pltpu.VMEM((more_z, cy) + tile, F32),
        pltpu.VMEM((cz, more_y) + tile, F32),
        pltpu.VMEM((more_z, more_y) + tile, F32),
        pltpu.VMEM((packed,) + tile, F32),
        pltpu.VMEM((8, 128), F32),
    ]
    scratch += [pltpu.VMEM((t, cols, 128), F32) for t in totals] * 2
    scratch += [
        pltpu.SemaphoreType.DMA((2 * sum(totals),)),
        pltpu.SemaphoreType.DMA((2 * sum(totals),)),
        pltpu.SemaphoreType.DMA((12,)),
        pltpu.SemaphoreType.DMA((12,)),
        pltpu.SemaphoreType.DMA((7,)),
        pltpu.SemaphoreType.DMA((7,)),
        pltpu.SemaphoreType.DMA((4,)),
    ]
    scratch += [pltpu.VMEM((own,) + tile, F32)] * 4
    vmem = pl.BlockSpec(memory_space=pltpu.VMEM)
    smem = pl.BlockSpec(memory_space=pltpu.SMEM)
    w, hw, gram, rayleigh = pl.pallas_call(
        functools.partial(kernel, sizes, groups, (cz, cy, cx, slots, nproj, cols)),
        out_shape=(
            jax.ShapeDtypeStruct((own,) + tile, F32),
            jax.ShapeDtypeStruct((own,) + tile, F32),
            jax.ShapeDtypeStruct((3 * cols, 3 * cols), F32),
            jax.ShapeDtypeStruct((3 * cols, 3 * cols), F32),
        ),
        in_specs=[smem] * 4 + [vmem] + [pl.BlockSpec(memory_space=pl.ANY)] * 4 + [vmem] * 2,
        out_specs=(vmem,) * 4,
        scratch_shapes=scratch,
        compiler_params=pltpu.CompilerParams(collective_id=0, has_side_effects=True),
    )(
        offsets[:, 0, 0, 0], extents[:, 0, 0, 0], atom_count[0], proj_count[0, 0], coupling[0, 0, 0],
        *turned, potential, projectors[0, 0, 0],
    )
    w, hw, gram, rayleigh = pl.pallas_call(
        put_out,
        out_shape=tuple(jax.ShapeDtypeStruct(b.shape, F32) for b in (w, hw, gram, rayleigh)),
        in_specs=[vmem] * 4,
        out_specs=(vmem,) * 4,
    )(w, hw, gram, rayleigh)
    w, hw = (jnp.transpose(b.reshape(cz, cy, cols, cx), (2, 0, 1, 3)) for b in (w, hw))
    return (w, hw, gram, rayleigh)


def solution(mesh):
    sizes = tuple(mesh.shape[a] for a in AXES)
    in_specs = (
        P(None, "gz", "gy", "gx"),
        P(None, "gz", "gy", "gx"),
        P(None, "gz", "gy", "gx"),
        P(None, "gz", "gy", "gx"),
        P("gz", "gy", "gx"),
        P("gz", "gy", "gx", None, None, None),
        P("gz", "gy", "gx", None, None, None),
        P("gz", "gy", "gx"),
        P("gz", "gy", "gx", None),
        P(None, "gz", "gy", "gx", None),
        P(None, "gz", "gy", "gx", None),
    )
    out_specs = (P(None, "gz", "gy", "gx"), P(None, "gz", "gy", "gx"), P(), P())
    return jax.shard_map(
        functools.partial(per_device, sizes),
        mesh=mesh, in_specs=in_specs, out_specs=out_specs, check_vma=False,
    )
```

```python
import functools

import jax
import jax.numpy as jnp
from jax import lax
from jax.experimental import pallas as pl
from jax.experimental.pallas import tpu as pltpu
from jax.sharding import PartitionSpec as P

BZ, BY, BX = 4, 4, 16
LAP_CENTER = -5369.0 / 1800.0
LAP_COEFFS = (12.0 / 7.0, -15.0 / 56.0, 10.0 / 189.0, -1.0 / 112.0, 2.0 / 1925.0, -1.0 / 16632.0)
MESH = pl.DeviceIdType.MESH
AXES = ("gz", "gy", "gx")
F32 = jnp.float32
BF16 = jnp.bfloat16
HP, HX, XX, PP, WW, HW = range(6)


def tiles_of(count):
    return -(-count // 8)


def kernel(
    sizes, groups, dims,
    off_ref, ext_ref, count_ref, proj_ref, d_ref, x_in, hx_in, p_in, hp_in, v_ref, beta_ref,
    w_ref, hw_ref, gram_ref, ray_ref, red1_ref,
    stack, zext, ybuf, zybuf, plow, phigh, xr, xl, frame, frame_x, halo_x,
    blo, bhi, pieces, nf, nh, spack, rz, ry, rzy, rx, wout,
    *rest,
):
    cz, cy, cx, slots, nproj, cols = dims
    nz, ny, nx = sizes
    n_red = len(groups)
    bufs = (rest[:n_red], rest[n_red : 2 * n_red])
    rest = rest[2 * n_red :]
    red_send, red_recv, halo_send, halo_recv, spill_send, spill_recv = rest[:6]
    load_sem, x_ref, hx_ref, p_ref, hp_ref = rest[6:]
    loads = []
    for i, (source, target) in enumerate(
        ((x_in, x_ref), (hx_in, hx_ref), (p_in, p_ref), (hp_in, hp_ref))
    ):
        loads.append(pltpu.make_async_copy(source, target, load_sem.at[i]))
        loads[-1].start()
    zi, yi, xi = (lax.axis_index(a) for a in AXES)
    size_of = dict(zip(AXES, sizes))
    here = dict(zip(AXES, (zi, yi, xi)))
    fz, fy = cz + BZ - 1, cy + BY - 1
    own = cz * cy
    lane = lax.broadcasted_iota(jnp.int32, (cols, 128), 1)

    def neighbour(dz, dy, dx):
        step = dict(zip(AXES, (dz, dy, dx)))
        return {a: lax.rem(here[a] + step[a] + size_of[a], size_of[a]) for a in AXES}

    def member(group, offset):
        total = 1
        index = 0
        for a in group:
            total *= size_of[a]
            index = index * size_of[a] + here[a]
        target = lax.rem(index + offset, total)
        device = {}
        for a in reversed(group):
            device[a] = lax.rem(target, size_of[a])
            target = target // size_of[a]
        return {a: device.get(a, here[a]) for a in AXES}, index, total

    octant = [(1, 0, 0), (0, 1, 0), (1, 1, 0), (0, 0, 1), (1, 0, 1), (0, 1, 1), (1, 1, 1)]
    barrier = pltpu.get_barrier_semaphore()
    greeted = 0
    for group in groups:
        total = member(group, 0)[2]
        for offset in range(1, total):
            pl.semaphore_signal(
                barrier, inc=1, device_id=member(group, offset)[0], device_id_type=MESH
            )
            greeted += 1
    for dz, dy, dx in octant:
        for sign in (1, -1):
            pl.semaphore_signal(
                barrier, inc=1, device_id=neighbour(sign * dz, sign * dy, sign * dx),
                device_id_type=MESH,
            )
            greeted += 1

    def split_store(kind, cell, value):
        high = value.astype(BF16)
        low = (value - high.astype(F32)).astype(BF16)
        start = cell * 128 if isinstance(cell, int) else pl.multiple_of(cell * 128, 128)
        stack[kind * 32 : kind * 32 + 32, pl.ds(start, 128)] = jnp.concatenate([high, low], 0)

    for load in loads:
        load.wait()

    @pl.loop(0, cz)
    def _(z):
        for y in range(cy):
            cell = z * cy + y
            split_store(HX, cell, hx_ref[cell])
            split_store(HP, cell, hp_ref[cell])
            split_store(XX, cell, x_ref[cell])
            split_store(PP, cell, p_ref[cell])

    def products(left, right_from, right_to, count=1):
        m = lax.dot_general(
            stack[left * 32 : (left + count) * 32, :],
            stack[right_from * 32 : right_to * 32, :],
            (((1,), (1,)), ((), ())),
            preferred_element_type=F32,
        )
        parts = [m[32 * i : 32 * i + cols] + m[32 * i + cols : 32 * i + 32] for i in range(count)]
        return parts if count > 1 else parts[0]

    def reduced(which, payload):
        base = which * sum(member(g, 0)[2] for g in groups)
        for phase, group in enumerate(groups):
            buf = bufs[which][phase]
            _, index, total = member(group, 0)
            buf[index] = payload
            if phase == 0 and which == 0:
                pl.semaphore_wait(barrier, greeted)
            copies = []
            for offset in range(1, total):
                copies.append(
                    pltpu.make_async_remote_copy(
                        src_ref=buf.at[index],
                        dst_ref=buf.at[index],
                        send_sem=red_send.at[base + offset],
                        recv_sem=red_recv.at[base + offset],
                        device_id=member(group, offset)[0],
                        device_id_type=MESH,
                    )
                )
                copies[-1].start()
            base += total
            yield None
            for copy in copies:
                copy.wait()
            payload = buf[0]
            for slot in range(1, total):
                payload = payload + buf[slot]
        yield payload

    def finish(steps):
        out = None
        for out in steps:
            pass
        return out

    hx_row, x_row, p_row = products(HX, HP, WW, 3)
    first = jnp.where((lane >= 32) & (lane < 64), pltpu.roll(hx_row, 96, 1), x_row)

    def paired(upper, lower):
        upper = upper + pltpu.roll(upper, 112, 1)
        lower = lower + pltpu.roll(lower, 112, 1)
        return jnp.where(lane % 32 < 16, upper, pltpu.roll(lower, 16, 1))

    reduction = reduced(0, paired(first, p_row))
    next(reduction)

    per_slot = BZ * BY * nproj
    lane_p = lax.broadcasted_iota(jnp.int32, (nproj, 128), 1)
    row_p = lax.broadcasted_iota(jnp.int32, (nproj, 128), 0)
    in_tile = 128 // BX
    for s in range(slots):
        ox = off_ref[2, 0, 0, 0, s]
        along = lax.rem(lane_p - ox + 128, 128)
        along = jnp.where(row_p < proj_ref[0, s], along, 128)
        low_side = lane_p >= ox
        live = s < count_ref[0, 0]
        for a in range(BZ):
            for b in range(BY):
                used = live & (a < ext_ref[0, 0, 0, 0, s]) & (b < ext_ref[1, 0, 0, 0, s])
                limit = jnp.where(used, jnp.minimum(ext_ref[2, 0, 0, 0, s], BX), 0)
                box = a * BY + b
                part = beta_ref[s, :, (box // in_tile) * 128 : (box // in_tile) * 128 + 128]
                part = pltpu.roll(part, lax.rem(ox + 128 - BX * (box % in_tile), 128), 1)
                part = jnp.where(along < limit, part, 0.0)
                row = s * per_slot + box * nproj
                blo[row : row + nproj, :] = jnp.where(low_side, part, 0.0)
                bhi[row : row + nproj, :] = jnp.where(low_side, 0.0, part)
    rim_y = BY + 2
    rim = (BZ + 2) * rim_y

    @pl.loop(0, slots)
    def _(s):
        for i in range(rim):
            if i < rim_y or i >= rim - rim_y or i % rim_y in (0, rim_y - 1):
                pieces[s * rim + i] = jnp.zeros(pieces.shape[1:], F32)

    sums1 = finish(reduction)
    red1_ref[...] = sums1
    matrix = jnp.concatenate([pltpu.roll(sums1, 64, 1), pltpu.roll(sums1, 96, 1)], 0)
    lane2 = lax.broadcasted_iota(jnp.int32, (2 * cols, 128), 1)
    matrix = jnp.where(lane2 < cols, matrix, 0.0)
    for k in range(0, cols, 2):
        row0, row1 = matrix[k : k + 1, :], matrix[k + 1 : k + 2, :]
        col0, col1 = matrix[:, k : k + 1], matrix[:, k + 1 : k + 2]
        a, b = matrix[k : k + 1, k : k + 1], matrix[k : k + 1, k + 1 : k + 2]
        c, d = matrix[k + 1 : k + 2, k : k + 1], matrix[k + 1 : k + 2, k + 1 : k + 2]
        ratio = c / a
        schur = d - ratio * b
        new1 = (col1 - col0 * (b / a)) / schur
        new0 = col0 / a - new1 * ratio
        rest_of = matrix - new0 * row0 - new1 * row1
        matrix = jnp.where(lane2 == k, new0, jnp.where(lane2 == k + 1, new1, rest_of))
    theta_t = matrix[cols:, :]
    theta_cols = [jnp.broadcast_to(theta_t[:, k : k + 1], (cols, 128)) for k in range(cols)]

    @pl.loop(0, cz)
    def _(z):
        for y in range(cy):
            cell = z * cy + y
            xs = x_ref[cell]
            value = hx_ref[cell]
            for k in range(cols):
                value = value - theta_cols[k] * xs[k : k + 1, :]
            vv = v_ref[z, y : y + 1, :]
            value = value / (1.0 + vv * vv)
            zext[cz + z, y] = value
            w_ref[cell] = value
            split_store(WW, cell, value)

    for q in range(tiles_of(own)):
        low = jnp.zeros((cols, 128), F32)
        high = low
        for j in range(min(8, own - 8 * q)):
            tile = zext[cz + (8 * q + j) // cy, (8 * q + j) % cy]
            keep = (lane >= 16 * j) & (lane < 16 * j + 16)
            low = jnp.where(keep, pltpu.roll(tile, 16 * j, 1) if j else tile, low)
            high = jnp.where(keep, pltpu.roll(tile, (16 * j + 16) % 128, 1) if j < 7 else tile, high)
        plow[q] = low
        phigh[q] = high

    two_y = ny == 2
    more_z, more_y = fz - cz, fy - cy
    z_tiles = tiles_of(more_z * cy)
    corner_tiles = tiles_of((more_z - 1) * cy + more_y)

    def some(ref, z, dz, y, dy):
        return ref.at[pl.ds(z, dz), pl.ds(y, dy)]

    def layers(target, base, z, dz, y, dy, where):
        return some(zext, cz + z, dz, y, dy), some(target, base + z, dz, y, dy), where

    early = [
        (some(zext, cz, more_z, 0, more_y), zybuf, (-1, -1, 0)),
        (plow.at[pl.ds(0, corner_tiles)], xr.at[3, pl.ds(0, corner_tiles)], (-1, -1, -1)),
        (plow, xr.at[2], (0, -1, -1)),
        (plow.at[pl.ds(0, z_tiles)], xr.at[1, pl.ds(0, z_tiles)], (-1, 0, -1)),
        (plow, xr.at[0], (0, 0, -1)),
        layers(ybuf.at[1], 0, 0, cz, 0, more_y, (0, -1, 0)),
        layers(zext, 2 * cz, 0, more_z, 0, cy, (-1, 0, 0)),
    ]
    late = [
        (phigh, xl, (0, 0, 1)),
        layers(ybuf.at[1], 0, 0, cz, more_y, cy - more_y, (0, -1, 0)),
        layers(zext, 2 * cz, more_z, cz - more_z, 0, cy, (-1, 0, 0)),
        layers(zext, 0, 0, cz, 0, cy, (1, 0, 0)),
    ]
    if not two_y:
        late.append(layers(ybuf.at[0], 0, 0, cz, 0, cy, (0, 1, 0)))

    def launch(sends, send_sem, recv_sem, first=0):
        copies = []
        for i, (source, target, where) in enumerate(sends, start=first):
            copies.append(
                pltpu.make_async_remote_copy(
                    src_ref=source,
                    dst_ref=target,
                    send_sem=send_sem.at[i],
                    recv_sem=recv_sem.at[i],
                    device_id=neighbour(*where),
                    device_id_type=MESH,
                )
            )
            copies[-1].start()
        return copies

    copies = launch(early, halo_send, halo_recv)
    late_copies = launch(late, halo_send, halo_recv, len(early))
    w_row = products(WW, HP, WW)
    w_row2 = products(WW, XX, HW)
    for copy in copies:
        copy.wait()

    below_y = 1 if two_y else 0
    for z in range(fz):
        for y in range(fy):
            up_z, up_y = z >= cz, y >= cy
            local = (z - cz * up_z) * cy + (y - cy * up_y)
            if up_z and up_y:
                tile = zybuf[z - cz, y - cy]
            elif up_z:
                tile = zext[cz + z, y]
            elif up_y:
                tile = ybuf[1, z, y - cy]
            else:
                tile = zext[cz + z, y]
            frame[z * fy + y] = tile
            shift = (128 - 16 * (local % 8)) % 128
            tile = xr[up_z + 2 * up_y, local // 8]
            tile = pltpu.roll(tile, shift, 1) if shift else tile
            frame_x[z * fy + y] = tile

    @pl.loop(0, slots)
    def _(s):
        oz, oy = off_ref[0, 0, 0, 0, s], off_ref[1, 0, 0, 0, s]
        sums = [jnp.zeros((cols, 128), F32) for _ in range(nproj)]
        for a in range(BZ):
            for b in range(BY):
                at = (oz + a) * fy + oy + b
                tile, tile_x = frame[at], frame_x[at]
                base = s * per_slot + (a * BY + b) * nproj
                for q in range(nproj):
                    sums[q] = sums[q] + tile * blo[pl.ds(base + q, 1), :]
                    sums[q] = sums[q] + jnp.where(
                        lane < 16, tile_x * bhi[pl.ds(base + q, 1), :], 0.0
                    )
        overlaps = [jnp.broadcast_to(jnp.sum(v, axis=1, keepdims=True), (cols, 128)) for v in sums]
        outs = []
        dm = d_ref[0, 0, 0, s]
        for p in range(nproj):
            value = overlaps[p] * dm[p : p + 1, p : p + 1]
            for q in range(nproj):
                if q != p:
                    value = value + overlaps[q] * (0.5 * (dm[p : p + 1, q : q + 1] + dm[q : q + 1, p : p + 1]))
            outs.append(value)
        for a in range(BZ):
            for b in range(BY):
                base = s * per_slot + (a * BY + b) * nproj
                low = outs[0] * blo[pl.ds(base, 1), :]
                high = outs[0] * bhi[pl.ds(base, 1), :]
                for p in range(1, nproj):
                    low = low + outs[p] * blo[pl.ds(base + p, 1), :]
                    high = high + outs[p] * bhi[pl.ds(base + p, 1), :]
                place = s * rim + (a + 1) * rim_y + b + 1
                pieces[place, 0] = low
                pieces[place, 1] = high

    @pl.loop(0, fz)
    def _(z):
        starts = []
        for s in range(slots):
            a = jnp.minimum(jnp.maximum(z - off_ref[0, 0, 0, 0, s], -1), BZ) + 1
            starts.append(s * rim + a * rim_y)
        for y in range(fy):
            low = jnp.zeros((cols, 128), F32)
            high = low
            for s in range(slots):
                b = jnp.minimum(jnp.maximum(y - off_ref[1, 0, 0, 0, s], -1), BY) + 1
                low = low + pieces[starts[s] + b, 0]
                high = high + pieces[starts[s] + b, 1]
            nf[z, y] = low
            nh[z, y] = high

    spans = []
    filled = 0
    for up_z in (0, 1):
        for up_y in (0, 1):
            cells = [
                (z, y)
                for z in (range(cz, fz) if up_z else range(cz))
                for y in (range(cy, fy) if up_y else range(cy))
            ]
            spans.append((filled, up_z, up_y, cells))
            for q in range(tiles_of(len(cells))):
                tile = jnp.zeros((cols, 128), F32)
                for j, (z, y) in enumerate(cells[8 * q : 8 * q + 8]):
                    keep = (lane >= 16 * j) & (lane < 16 * j + 16)
                    value = nh[z, y]
                    tile = jnp.where(keep, pltpu.roll(value, 16 * j, 1) if j else value, tile)
                spack[filled + q] = tile
            filled += tiles_of(len(cells))
    sends = [
        (nf.at[pl.ds(cz, more_z), pl.ds(0, cy)], rz, (1, 0, 0)),
        (nf.at[pl.ds(0, cz), pl.ds(cy, more_y)], ry, (0, 1, 0)),
        (nf.at[pl.ds(cz, more_z), pl.ds(cy, more_y)], rzy, (1, 1, 0)),
    ]
    for begin, up_z, up_y, cells in spans:
        part = pl.ds(begin, tiles_of(len(cells)))
        sends.append((spack.at[part], rx.at[part], (up_z, up_y, 1)))
    copies = launch(sends, spill_send, spill_recv)

    for copy in late_copies:
        copy.wait()
    for cell in range(own):
        turn = (112 - 16 * (cell % 8)) % 128
        left = xl[cell // 8]
        left = pltpu.roll(left, turn, 1) if turn else left
        halo_x[cell] = jnp.where(lane < 64, frame_x[cell // cy * fy + cell % cy], left)

    @pl.loop(0, cz)
    def _(z):
        for y in range(cy):
            cell = z * cy + y
            centre = zext[cz + z, y]
            edge = halo_x[cell]
            vv = v_ref[z, y : y + 1, :]
            total = centre * (vv - 1.5 * LAP_CENTER)
            for k, weight in enumerate(LAP_COEFFS, start=1):
                beside = zext[cz + z + k, y] + zext[cz + z - k, y]
                for target in (y + k, y - k):
                    if target >= cy:
                        beside = beside + ybuf[1, z, target - cy]
                    elif target < 0:
                        beside = beside + ybuf[below_y, z, target + cy]
                    else:
                        beside = beside + zext[cz + z, target]
                beside = beside + pltpu.roll(jnp.where(lane < k, edge, centre), 128 - k, 1)
                beside = beside + pltpu.roll(jnp.where(lane >= 128 - k, edge, centre), k, 1)
                total = total - 0.5 * weight * beside
            hw_ref[cell] = total + nf[z, y]

    for copy in copies:
        copy.wait()
    for z in range(cz):
        for y in range(cy):
            cell = z * cy + y
            value = hw_ref[cell]
            if z < more_z:
                value = value + rz[z, y]
            if y < more_y:
                value = value + ry[z, y]
            if z < more_z and y < more_y:
                value = value + rzy[z, y]
            extra = None
            for begin, up_z, up_y, cells in spans:
                where = (z + cz * up_z, y + cy * up_y)
                if where in cells:
                    index = cells.index(where)
                    tile = rx[begin + index // 8]
                    shift = (128 - 16 * (index % 8)) % 128
                    tile = pltpu.roll(tile, shift, 1) if shift else tile
                    extra = tile if extra is None else extra + tile
            value = value + jnp.where(lane < 16, extra, 0.0)
            hw_ref[cell] = value
            split_store(HW, cell, value)

    hw_row = products(HW, XX, HW + 1)
    second = jnp.where(lane < 96, hw_row, pltpu.roll(w_row2_pad(w_row2), 32, 1))
    sums2 = finish(reduced(1, paired(w_row, second)))
    weight = 1.0 / (own * cx * nz * ny * nx)
    sums1 = red1_ref[...]
    rows = jnp.concatenate([sums1, pltpu.roll(sums1, 112, 1), sums2, pltpu.roll(sums2, 112, 1)], 0)
    rows = rows * weight
    turned = jnp.transpose(jnp.concatenate([rows, jnp.zeros_like(rows)], 0))

    def direct(row, group, target):
        return rows[16 * row : 16 * row + 16, :], 32 * group, target

    def flipped(row, group, target):
        return turned[32 * group : 32 * group + 16, :], 16 * row, target

    def laid(parts):
        total = None
        for tile, begin, target in parts:
            shift = (16 * target - begin) % 128
            tile = pltpu.roll(tile, shift, 1) if shift else tile
            tile = jnp.where((lane >= 16 * target) & (lane < 16 * target + 16), tile, 0.0)
            total = tile if total is None else total + tile
        return total

    gram = [
        [direct(0, 2, 0), flipped(2, 2, 1), direct(0, 3, 2)],
        [direct(2, 2, 0), direct(3, 3, 1), direct(2, 3, 2)],
        [direct(1, 2, 0), flipped(2, 3, 1), direct(1, 3, 2)],
    ]
    rayleigh = [
        [flipped(0, 1, 0), flipped(3, 0, 1), direct(0, 0, 2)],
        [direct(2, 1, 0), flipped(3, 2, 1), direct(2, 0, 2)],
        [direct(1, 1, 0), flipped(3, 1, 1), direct(1, 0, 2)],
    ]
    for i in range(3):
        gram_ref[16 * i : 16 * i + 16, :] = laid(gram[i])[:, :48]
        ray_ref[16 * i : 16 * i + 16, :] = laid(rayleigh[i])[:, :48]


def put_out(*refs):
    half = len(refs) // 2
    for source, target in zip(refs[:half], refs[half:]):
        target[...] = source[...]


def w_row2_pad(row):
    return jnp.concatenate([row, jnp.zeros((row.shape[0], 128 - row.shape[1]), row.dtype)], 1)


def per_device(
    sizes,
    block_x, block_hx, block_p, block_hp, potential, projectors, coupling,
    atom_count, proj_count, offsets, extents,
):
    cols, cz, cy, cx = block_x.shape
    slots, nproj = projectors.shape[-3], projectors.shape[-2]
    nz, ny, nx = sizes
    own = cz * cy
    fz, fy = cz + BZ - 1, cy + BY - 1
    turned = [
        jnp.transpose(b, (1, 2, 0, 3)).reshape(own, cols, cx)
        for b in (block_x, block_hx, block_p, block_hp)
    ]
    groups = (("gz", "gy"), ("gx",)) if nz * ny <= 16 else (("gz",), ("gy",), ("gx",))
    size_of = dict(zip(AXES, sizes))
    totals = []
    for group in groups:
        total = 1
        for a in group:
            total *= size_of[a]
        totals.append(total)
    tile = (cols, 128)
    more_z, more_y = fz - cz, fy - cy
    packed = sum(
        tiles_of(zc * yc) for zc in (cz, more_z) for yc in (cy, more_y)
    )
    per_slot = BZ * BY * nproj
    scratch = [
        pltpu.VMEM((cols, 128), F32),
        pltpu.VMEM((192, own * 128), BF16),
        pltpu.VMEM((3 * cz, cy) + tile, F32),
        pltpu.VMEM((2, cz, cy) + tile, F32),
        pltpu.VMEM((BZ - 1, BY - 1) + tile, F32),
        pltpu.VMEM((tiles_of(own),) + tile, F32),
        pltpu.VMEM((tiles_of(own),) + tile, F32),
        pltpu.VMEM((4, tiles_of(own)) + tile, F32),
        pltpu.VMEM((tiles_of(own),) + tile, F32),
        pltpu.VMEM((fz * fy,) + tile, F32),
        pltpu.VMEM((fz * fy,) + tile, F32),
        pltpu.VMEM((own,) + tile, F32),
        pltpu.VMEM((slots * per_slot, 128), F32),
        pltpu.VMEM((slots * per_slot, 128), F32),
        pltpu.VMEM((slots * (BZ + 2) * (BY + 2), 2) + tile, F32),
        pltpu.VMEM((fz, fy) + tile, F32),
        pltpu.VMEM((fz, fy) + tile, F32),
        pltpu.VMEM((packed,) + tile, F32),
        pltpu.VMEM((more_z, cy) + tile, F32),
        pltpu.VMEM((cz, more_y) + tile, F32),
        pltpu.VMEM((more_z, more_y) + tile, F32),
        pltpu.VMEM((packed,) + tile, F32),
        pltpu.VMEM((8, 128), F32),
    ]
    scratch += [pltpu.VMEM((t, cols, 128), F32) for t in totals] * 2
    scratch += [
        pltpu.SemaphoreType.DMA((2 * sum(totals),)),
        pltpu.SemaphoreType.DMA((2 * sum(totals),)),
        pltpu.SemaphoreType.DMA((12,)),
        pltpu.SemaphoreType.DMA((12,)),
        pltpu.SemaphoreType.DMA((7,)),
        pltpu.SemaphoreType.DMA((7,)),
        pltpu.SemaphoreType.DMA((4,)),
    ]
    scratch += [pltpu.VMEM((own,) + tile, F32)] * 4
    vmem = pl.BlockSpec(memory_space=pltpu.VMEM)
    smem = pl.BlockSpec(memory_space=pltpu.SMEM)
    w, hw, gram, rayleigh = pl.pallas_call(
        functools.partial(kernel, sizes, groups, (cz, cy, cx, slots, nproj, cols)),
        out_shape=(
            jax.ShapeDtypeStruct((own,) + tile, F32),
            jax.ShapeDtypeStruct((own,) + tile, F32),
            jax.ShapeDtypeStruct((3 * cols, 3 * cols), F32),
            jax.ShapeDtypeStruct((3 * cols, 3 * cols), F32),
        ),
        in_specs=[smem] * 4 + [vmem] + [pl.BlockSpec(memory_space=pl.ANY)] * 4 + [vmem] * 2,
        out_specs=(vmem,) * 4,
        scratch_shapes=scratch,
        compiler_params=pltpu.CompilerParams(collective_id=0, has_side_effects=True),
    )(
        offsets, extents, atom_count[0], proj_count[0, 0], coupling,
        *turned, potential, projectors[0, 0, 0],
    )
    w, hw, gram, rayleigh = pl.pallas_call(
        put_out,
        out_shape=tuple(jax.ShapeDtypeStruct(b.shape, F32) for b in (w, hw, gram, rayleigh)),
        in_specs=[vmem] * 4,
        out_specs=(vmem,) * 4,
    )(w, hw, gram, rayleigh)
    w, hw = (jnp.transpose(b.reshape(cz, cy, cols, cx), (2, 0, 1, 3)) for b in (w, hw))
    return (w, hw, gram, rayleigh)


def solution(mesh):
    sizes = tuple(mesh.shape[a] for a in AXES)
    in_specs = (
        P(None, "gz", "gy", "gx"),
        P(None, "gz", "gy", "gx"),
        P(None, "gz", "gy", "gx"),
        P(None, "gz", "gy", "gx"),
        P("gz", "gy", "gx"),
        P("gz", "gy", "gx", None, None, None),
        P("gz", "gy", "gx", None, None, None),
        P("gz", "gy", "gx"),
        P("gz", "gy", "gx", None),
        P(None, "gz", "gy", "gx", None),
        P(None, "gz", "gy", "gx", None),
    )
    out_specs = (P(None, "gz", "gy", "gx"), P(None, "gz", "gy", "gx"), P(), P())
    return jax.shard_map(
        functools.partial(per_device, sizes),
        mesh=mesh, in_specs=in_specs, out_specs=out_specs, check_vma=False,
    )
```
